32 devices in a mesh: tm: 8 (over z, y), mp: 4 (over x, core).
Axes of the slice: x: 2, y: 2, z: 4, core: 2. Of those that a mesh axis runs over, the one named last changes fastest.
Arguments:
- latents: float32 [4, 8, 4, 4096], P(None, 'tm'), may hold values from -6 to 6
- noise: float32 [4, 8, 4, 4096], P(None, 'tm'), may hold values from -6 to 6
- start_step: int32 [4], replicated, may hold values from 8 to 999
- slide: int32 [4], replicated, may hold values from 1 to 8, as said below
- w_in: float32 [4, 320], replicated, may hold values from -3 to 3
- w_gate: bfloat16 [320, 1280], P(None, 'mp'), may hold values from -0.3125 to 0.3125
- w_value: bfloat16 [320, 1280], P(None, 'mp'), may hold values from -0.3125 to 0.3125
- w_down: bfloat16 [1280, 320], P('mp'), may hold values from -0.15625 to 0.15625
- w_out: float32 [320, 4], replicated, may hold values from -0.3125 to 0.3125
Outputs:
- next_window: float32 [4, 8, 4, 4096], P(None, 'tm')
- eps: float32 [4, 8, 4, 4096], P(None, 'tm', None, 'mp')
The draws below stay inside these ranges and needn't reach their ends.
Inputs may be any that keep to these rules, and one draw needn't show every extreme that they name: `slide`: some prompt slides by exactly 8, and another by exactly 1.
All inputs are finite; a program needn't handle non-finite values.
Results may differ from the reference program's by a relative error of at most 0.0023.
Values sent between devices are 32-bit elements; how exact they have to be, the bound alone decides.
A program may use at most 64 MiB of HBM per device.

```python
import math
import jax
import jax.numpy as jnp
from jax import lax

C = 320
FF = 1280
LAT = 4
POS = 4096
PROMPTS = 4
TSTEPS = 1000
WIN = 8
SMAX = 8


def draw_slide(key, part):
    first, second = jax.random.split(jax.random.fold_in(key, 17))
    values = jax.random.randint(first, (PROMPTS,), 1, SMAX + 1)
    order = jax.random.permutation(second, PROMPTS)
    values = jnp.where(order == 0, SMAX, values)
    values = jnp.where(order == 1, 1, values)
    return values.astype(jnp.int32)


def plant(array, own_key, low, top_value):
    longest = array.shape.index(max(array.shape))
    spots = []
    for shift in (0, 1):
        where = [jax.random.randint(jax.random.fold_in(own_key, axis), (), 0, length) for axis, length in enumerate(array.shape)]
        where[longest] = (where[longest] + shift) % array.shape[longest]
        spots.append(tuple(where))
    return array.at[spots[0]].set(low).at[spots[1]].set(top_value)


def block_levels(key, dims, cuts, least, largest):
    level, own = 1.0, jax.random.fold_in(key, 6)
    for position, shards_of in cuts:
        steps = jnp.exp(jax.random.uniform(jax.random.fold_in(own, position), (shards_of,), jnp.float32, least / len(cuts), largest / len(cuts)))
        level = level * jnp.repeat(steps, dims[position] // shards_of).reshape([-1 if axis == position else 1 for axis in range(len(dims))])
    return level


def bell_draw(rng, extent, deviation, bound, pieces=(), kind=jnp.bfloat16):
    loudness = block_levels(rng, extent, pieces, -0.22, 0.18) if pieces else 1.0
    entries = jax.random.normal(rng, extent, jnp.float32) * deviation * loudness
    return jnp.minimum(jnp.maximum(entries, -bound), bound).astype(kind)


def setup_inputs(seed: int = 0) -> dict:
    splits = jax.random.split(jax.random.key(seed), 10)
    latents = bell_draw(splits[0], (PROMPTS, WIN, LAT, POS), 1.0, 6.0, ((1, 8),), jnp.float32)
    noise = bell_draw(splits[1], (PROMPTS, WIN, LAT, POS), 1.0, 6.0, ((1, 8),), jnp.float32)
    start_step = plant(jax.random.randint(splits[2], (PROMPTS,), WIN, TSTEPS), jax.random.fold_in(splits[2], 1), WIN, TSTEPS - 1).astype(jnp.int32)
    slide = draw_slide(jax.random.fold_in(splits[9], 71), 0)
    w_in = bell_draw(splits[4], (LAT, C), LAT ** -0.5, 3.0, (), jnp.float32)
    w_gate = bell_draw(splits[5], (C, FF), C ** -0.5, 0.3125, ((1, 4),))
    w_value = bell_draw(splits[6], (C, FF), C ** -0.5, 0.3125, ((1, 4),))
    w_down = bell_draw(splits[7], (FF, C), FF ** -0.5, 0.15625, ((0, 4),))
    w_out = bell_draw(splits[8], (C, LAT), C ** -0.5, 0.3125, (), jnp.float32)
    return {"latents": latents, "noise": noise, "start_step": start_step, "slide": slide, "w_in": w_in, "w_gate": w_gate, "w_value": w_value, "w_down": w_down, "w_out": w_out}


def plan():
    steps_f = jnp.arange(TSTEPS, dtype=jnp.float32)
    beta = 0.0001 + (0.02 - 0.0001) * steps_f / (TSTEPS - 1)
    abar = jnp.cumprod(1.0 - beta)
    return (beta, abar)

def embed(times):
    half = C // 2
    freq = jnp.exp(-math.log(10000.0) * jnp.arange(half, dtype=jnp.float32) / half)
    angle = times[..., None] * freq
    return jnp.concatenate([jnp.cos(angle), jnp.sin(angle)], axis=-1)

def reference(latents, noise, start_step, slide, w_in, w_gate, w_value, w_down, w_out):
    beta, abar = plan()
    slots = jnp.arange(WIN, dtype=jnp.int32)
    times = start_step[:, None] - slots[None, :]
    beta_t = beta[times][:, :, None, None]
    abar_t = abar[times][:, :, None, None]
    emb = embed(times.astype(jnp.float32)).reshape(PROMPTS * WIN, C)
    items = latents.reshape(PROMPTS * WIN, LAT, POS)

    def denoise(pair):
        latent, vector = pair
        hid = jnp.dot(w_in.T, latent, precision=lax.Precision.HIGHEST) + vector[:, None]
        mean = lax.optimization_barrier(jnp.mean(hid, axis=0))
        var = lax.optimization_barrier(jnp.mean((hid - mean) ** 2, axis=0))
        normed = ((hid - mean) * lax.rsqrt(var + 1e-05)).astype(jnp.bfloat16)
        gate = jnp.dot(w_gate.T, normed, preferred_element_type=jnp.float32)
        value = jnp.dot(w_value.T, normed, preferred_element_type=jnp.float32)
        hidden = (jax.nn.gelu(gate, approximate=False) * value).astype(jnp.bfloat16)
        branch = jnp.dot(w_down.T, hidden, preferred_element_type=jnp.float32)
        return jnp.dot(w_out.T, hid + branch, precision=lax.Precision.HIGHEST)
    eps = lax.map(denoise, (items, emb)).reshape(PROMPTS, WIN, LAT, POS)
    stepped = (latents - beta_t / jnp.sqrt(1.0 - abar_t) * eps) / jnp.sqrt(1.0 - beta_t) + jnp.sqrt(beta_t) * noise
    drift = stepped - latents
    updated = latents[:, :1] + (jnp.cumsum(drift, axis=1) - drift)
    source = jnp.minimum(slots[None, :] + slide[:, None], WIN - 1).astype(jnp.int32)
    next_window = jnp.take_along_axis(updated, source[:, :, None, None], axis=1)
    return (next_window, eps)
```

```python
import functools
import math

import jax
import jax.numpy as jnp
import numpy as np
from jax import lax
from jax.experimental import pallas as pl
from jax.experimental.pallas import tpu as pltpu
from jax.sharding import PartitionSpec as P

TSTEPS = 1000
F32, BF16 = jnp.float32, jnp.bfloat16
HIGH = lax.Precision.HIGHEST


def step_table(channels):
    beta = 1e-4 + (0.02 - 1e-4) * np.arange(TSTEPS, dtype=np.float64) / (TSTEPS - 1)
    abar = np.cumprod(1.0 - beta)
    root = np.sqrt(1.0 - beta)
    half = channels // 2
    freq = np.exp(-math.log(10000.0) * np.arange(half, dtype=np.float64) / half)
    table = np.zeros((4, max(TSTEPS, channels)), np.float32)
    table[:3, :TSTEPS] = [1.0 / root - 1.0, beta / np.sqrt(1.0 - abar) / root, np.sqrt(beta)]
    table[3, :channels] = np.concatenate([freq, freq])
    return table


def split3(v):
    a = v.astype(BF16).astype(F32)
    rest = v - a
    b = rest.astype(BF16).astype(F32)
    return a, b, rest - b


def six(parts, left):
    a, b, c = parts
    return jnp.concatenate([a, b, c, a, b, a] if left else [a, a, a, b, b, c], axis=0)


def contract(a, b, da, db, **kw):
    return lax.dot_general(a, b, (((da,), (db,)), ((), ())), preferred_element_type=F32, **kw)


def kernel(n_tm, n_mp, width, x_hbm, z_hbm, start_ref, slide_ref, table_hbm, win_hbm, wg_hbm, wv_hbm, wd_hbm, wo_hbm,
           out_ref, eps_ref, x_ref, z_ref, table_ref, win_ref, wg_ref, wv_ref, wd_ref, wo_ref, load, hid, wbuf, a_scr, f_scr, y_scr, dbuf, obuf, pbuf,
           coef, wsend, wrecv, dsend, drecv, psend, osend, precv):
    prompts, _, lat, pos = x_hbm.shape
    units = wg_ref.shape[1]
    rank = lat + prompts
    share = pos // n_mp
    cuts = share // width
    pieces = prompts * cuts
    n_z = n_tm // 2
    tm, mp = lax.axis_index("tm"), lax.axis_index("mp")
    zi, yi = lax.div(tm, 2), lax.rem(tm, 2)
    twin = tm + 1 - 2 * yi
    mesh_id = pl.DeviceIdType.MESH
    cols = pl.ds(pl.multiple_of(mp * share, 128), share)

    pairs = [(win_hbm, win_ref), (table_hbm, table_ref), (wg_hbm, wg_ref), (wv_hbm, wv_ref), (wo_hbm, wo_ref),
             (wd_hbm, wd_ref), (x_hbm.at[:, :, :, cols], x_ref), (z_hbm.at[:, :, :, cols], z_ref)]
    loads = [pltpu.make_async_copy(a, b, load.at[i]) for i, (a, b) in enumerate(pairs)]
    for one in loads:
        one.start()
    barrier = pltpu.get_barrier_semaphore()

    def over_z(op):
        lax.fori_loop(0, n_z - 1, lambda k, c: (op(k, k + jnp.where(k >= zi, 1, 0)), c)[1], 0)

    def greet(device):
        pl.semaphore_signal(barrier, inc=1, device_id=device, device_id_type=mesh_id)

    over_z(lambda k, z: greet({"tm": 2 * z + yi}))
    for k in range(1, n_mp):
        greet({"mp": lax.rem(mp + k, n_mp)})
    for k in range(n_mp):
        greet({"tm": twin, "mp": lax.rem(mp + k, n_mp)})

    for one in loads[:6]:
        one.wait()
    channels = win_ref.shape[1]
    order = lax.broadcasted_iota(jnp.int32, (prompts, channels), 0)
    times = jnp.zeros((prompts, channels), F32)
    for p in range(prompts):
        times = jnp.where(order == p, (start_ref[p] - tm).astype(F32), times)
    angle = times * table_ref[3:4, :channels]
    lane = lax.broadcasted_iota(jnp.int32, (prompts, channels), 1)
    emb = jnp.where(lane < channels // 2, jnp.cos(angle), jnp.sin(angle))
    raw = jnp.concatenate([win_ref[...], emb], axis=0)
    left = raw - jnp.mean(raw, axis=1, keepdims=True)
    l3 = jnp.concatenate(split3(left), axis=0).astype(BF16)

    def folded(weights, width, db):
        got = contract(l3 if db == 0 else o3, weights, 1, db)
        return got[:width] + got[width:2 * width] + got[2 * width:3 * width]

    wot = wo_ref[...]
    o3 = jnp.concatenate(split3(wot) + (jnp.zeros_like(wot),), axis=0).astype(BF16)
    root = math.sqrt(0.5)
    wbuf[0, 0:rank] = folded(wg_ref[...], rank, 0) * root
    wbuf[0, rank:2 * rank] = folded(wv_ref[...], rank, 0) * root
    wbuf[0, 2 * rank:2 * rank + lat] = folded(wd_ref[...], lat, 1)

    pl.semaphore_wait(barrier, n_z + 2 * n_mp - 2)

    def table_copy(k):
        return pltpu.make_async_remote_copy(
            wbuf.at[0], wbuf.at[n_mp - k], wsend.at[k], wrecv.at[n_mp - k],
            device_id={"mp": lax.rem(mp + k, n_mp)}, device_id_type=mesh_id)

    for k in range(1, n_mp):
        table_copy(k).start()

    def build(k):
        for part in range(2):
            a, b, c = split3(wbuf[k, part * rank:(part + 1) * rank])
            a_scr[k, part * units:(part + 1) * units] = six((a, b, c), True).T.astype(BF16)
        a, b, c = split3(wbuf[k, 2 * rank:2 * rank + lat])
        f_scr[:, k * units:(k + 1) * units] = jnp.concatenate([a, b, c, jnp.zeros_like(a)], axis=0).astype(BF16)

    grid = lax.broadcasted_iota(jnp.int32, table_ref.shape, 1)
    for p in range(prompts):
        picked = jnp.where(grid == start_ref[p] - tm, table_ref[...], 0.0)
        coef[p] = jnp.broadcast_to(jnp.sum(picked, axis=1, keepdims=True), coef.shape[1:])

    base = contract(raw, wot, 1, 1, precision=HIGH)
    base6 = six(split3(base), True).T.astype(BF16)
    left6 = six(split3(left), True).T.astype(BF16)
    rows = lax.broadcasted_iota(jnp.int32, (prompts, share), 0)
    for one in loads[6:]:
        one.wait()
    for p in range(prompts):
        u = jnp.concatenate([x_ref[p, 0], (rows == p).astype(F32)], axis=0)
        u6 = six(split3(u), False).astype(BF16)
        hc = jnp.dot(left6, u6, preferred_element_type=F32)
        eps_ref[p, 0] = jnp.dot(base6, u6, preferred_element_type=F32)
        var = jnp.mean(hc * hc, axis=0, keepdims=True)
        y_scr[p] = six(split3(u * lax.rsqrt(var + 1e-5)), False).astype(BF16)

    def split(q):
        return lax.div(q, cuts), pl.ds(pl.multiple_of(lax.rem(q, cuts) * width, 128), width)

    def sweep(q, chunks):
        p, at = split(q)
        yt = y_scr[p, :, at]
        for k in chunks:
            gate = jnp.dot(a_scr[k, :units], yt, preferred_element_type=F32)
            value = jnp.dot(a_scr[k, units:], yt, preferred_element_type=F32)
            hid[p, k * units:(k + 1) * units, at] = ((gate * (1.0 + lax.erf(gate))) * value).astype(BF16)

    def drift_copy(q, k, z):
        return pltpu.make_async_remote_copy(
            dbuf.at[zi, q], dbuf.at[zi, q], dsend.at[k, q], drecv.at[zi, q],
            device_id={"tm": 2 * z + yi}, device_id_type=mesh_id)

    def drift_arrival(q, k, z):
        return pltpu.make_async_remote_copy(
            dbuf.at[z, q], dbuf.at[z, q], dsend.at[k, q], drecv.at[z, q],
            device_id={"tm": 2 * z + yi}, device_id_type=mesh_id)

    def step(q):
        p, at = split(q)
        got = jnp.dot(f_scr[...], hid[p, :, at], preferred_element_type=F32)
        eps = eps_ref[p, 0, :, at] + got[:lat] + got[lat:2 * lat] + got[2 * lat:3 * lat]
        eps_ref[p, 0, :, at] = eps
        x = x_ref[p, 0, :, at]
        c = coef[p]
        term = c[0:1, :1] * x - c[1:2, :1] * eps + c[2:3, :1] * z_ref[p, 0, :, at]
        dbuf[zi, q] = term + jnp.where(tm == 0, 1.0, 0.0) * x
        over_z(lambda k, z: drift_copy(q, k, z).start())

    def place(q, peer):
        return pl.ds(pl.multiple_of(peer * share + lax.rem(q, cuts) * width, 128), width)

    def own_copy(q, k):
        spot = pbuf.at[yi, lax.div(q, cuts), :, place(q, mp)]
        return pltpu.make_async_remote_copy(
            spot, spot, psend.at[k, q], precv.at[yi, mp, q],
            device_id={"mp": lax.rem(mp + k, n_mp)}, device_id_type=mesh_id)

    def twin_copy(q, k):
        spot = pbuf.at[yi, lax.div(q, cuts), :, place(q, mp)]
        return pltpu.make_async_remote_copy(
            obuf.at[q], spot, osend.at[k, q], precv.at[yi, mp, q],
            device_id={"tm": twin, "mp": lax.rem(mp + k, n_mp)}, device_id_type=mesh_id)

    def arrival(q, side, k):
        peer = lax.rem(mp + k, n_mp)
        spot = pbuf.at[side, lax.div(q, cuts), :, place(q, peer)]
        return pltpu.make_async_remote_copy(
            spot, spot, psend.at[k, q], precv.at[side, peer, q],
            device_id={"mp": lax.rem(mp + 1, n_mp)}, device_id_type=mesh_id)

    def finish(q):
        over_z(lambda k, z: drift_arrival(q, k, z).wait_recv())
        p = lax.div(q, cuts)
        mine = jnp.minimum(tm + slide_ref[p], n_tm - 1)
        theirs = jnp.minimum(twin + slide_ref[p], n_tm - 1)

        def add(z, totals):
            part = dbuf[z, q]
            slot = 2 * z + yi
            return (totals[0] + jnp.where(slot < mine, 1.0, 0.0) * part,
                    totals[1] + jnp.where(slot < theirs, 1.0, 0.0) * part)

        zero = jnp.zeros((lat, width), F32)
        keep, give = lax.fori_loop(0, n_z, add, (zero, zero), unroll=n_z <= 8)
        pbuf[yi, p, :, place(q, mp)] = keep
        obuf[q] = give
        for k in range(n_mp):
            twin_copy(q, k).start()
        for k in range(1, n_mp):
            own_copy(q, k).start()

    def loop(count, op):
        lax.fori_loop(0, count, lambda q, c: (op(q), c)[1], 0)

    build(0)
    loop(pieces, lambda q: sweep(q, (0,)))
    for k in range(1, n_mp):
        table_copy(n_mp - k).wait_recv()
        build(k)

    def lap(q):
        sweep(q, range(1, n_mp))
        step(q)

    loop(pieces, lap)
    loop(pieces, finish)

    def settle(p):
        for c in range(cuts):
            q = p * cuts + c
            for k in range(n_mp):
                arrival(q, 1 - yi, k).wait_recv()
            for k in range(1, n_mp):
                arrival(q, yi, k).wait_recv()
        out_ref[p, 0] = pbuf[0, p] + pbuf[1, p]

    loop(prompts, settle)
    for k in range(1, n_mp):
        table_copy(k).wait_send()

    def drain(q):
        over_z(lambda k, z: drift_copy(q, k, z).wait_send())
        for k in range(n_mp):
            twin_copy(q, k).wait_send()
        for k in range(1, n_mp):
            own_copy(q, k).wait_send()

    loop(pieces, drain)


def shards(n_tm, n_mp, latents, noise, start_step, slide, w_in, w_gate, w_value, w_down, w_out):
    prompts, t_dev, lat, pos = latents.shape
    channels, units = w_gate.shape
    share = pos // n_mp
    rank = lat + prompts
    width = 512
    pieces = prompts * share // width
    n_z = n_tm // 2
    assert t_dev == 1 and n_tm % 2 == 0
    vmem = pl.BlockSpec(memory_space=pltpu.VMEM)
    smem = pl.BlockSpec(memory_space=pltpu.SMEM)
    dma = pltpu.SemaphoreType.DMA
    hbm = pl.BlockSpec(memory_space=pltpu.HBM)
    table = step_table(channels)
    return pl.pallas_call(
        functools.partial(kernel, n_tm, n_mp, width),
        out_shape=(pltpu.VMEM(latents.shape, F32), pltpu.VMEM((prompts, 1, lat, share), F32)),
        in_specs=[hbm, hbm, smem, smem] + [hbm] * 6,
        out_specs=(vmem, vmem),
        scratch_shapes=[
            pltpu.VMEM((prompts, 1, lat, share), F32),
            pltpu.VMEM((prompts, 1, lat, share), F32),
            pltpu.VMEM(table.shape, F32),
            pltpu.VMEM(w_in.shape, F32),
            pltpu.VMEM(w_gate.shape, BF16),
            pltpu.VMEM(w_value.shape, BF16),
            pltpu.VMEM(w_down.shape, BF16),
            pltpu.VMEM(w_in.shape, F32),
            dma((8,)),
            pltpu.VMEM((prompts, n_mp * units, share), BF16),
            pltpu.VMEM((n_mp, 2 * rank + 8, units), F32),
            pltpu.VMEM((n_mp, 2 * units, 6 * rank), BF16),
            pltpu.VMEM((4 * lat, n_mp * units), BF16),
            pltpu.VMEM((prompts, 6 * rank, share), BF16),
            pltpu.VMEM((n_z, pieces, lat, width), F32),
            pltpu.VMEM((pieces, lat, width), F32),
            pltpu.VMEM((2, prompts, lat, pos), F32),
            pltpu.VMEM((prompts, 4, 128), F32),
            dma((n_mp,)), dma((n_mp,)),
            dma((n_z, pieces)), dma((n_z, pieces)),
            dma((n_mp, pieces)), dma((n_mp, pieces)), dma((2, n_mp, pieces)),
        ],
        compiler_params=pltpu.CompilerParams(collective_id=0, has_side_effects=True, vmem_limit_bytes=60000 * 1024),
    )(latents, noise, start_step, slide, table, w_in, w_gate, w_value, w_down, w_out.T)


def solution(mesh):
    in_specs = (
        P(None, "tm", None, None),
        P(None, "tm", None, None),
        P(),
        P(),
        P(),
        P(None, "mp"),
        P(None, "mp"),
        P("mp", None),
        P(),
    )
    out_specs = (P(None, "tm", None, None), P(None, "tm", None, "mp"))
    body = functools.partial(shards, mesh.shape["tm"], mesh.shape["mp"])
    return jax.shard_map(body, mesh=mesh, in_specs=in_specs, out_specs=out_specs, check_vma=False)
```

```python
import functools
import math

import jax
import jax.numpy as jnp
import numpy as np
from jax import lax
from jax.experimental import pallas as pl
from jax.experimental.pallas import tpu as pltpu
from jax.sharding import PartitionSpec as P

TSTEPS = 1000
F32, BF16 = jnp.float32, jnp.bfloat16
HIGH = lax.Precision.HIGHEST


def step_table(channels):
    beta = 1e-4 + (0.02 - 1e-4) * np.arange(TSTEPS, dtype=np.float64) / (TSTEPS - 1)
    abar = np.cumprod(1.0 - beta)
    root = np.sqrt(1.0 - beta)
    half = channels // 2
    freq = np.exp(-math.log(10000.0) * np.arange(half, dtype=np.float64) / half)
    table = np.zeros((4, max(TSTEPS, channels)), np.float32)
    table[:3, :TSTEPS] = [1.0 / root - 1.0, beta / np.sqrt(1.0 - abar) / root, np.sqrt(beta)]
    table[3, :channels] = np.concatenate([freq, freq])
    return table


def split3(v):
    a = v.astype(BF16).astype(F32)
    rest = v - a
    b = rest.astype(BF16).astype(F32)
    return a, b, rest - b


def six(parts, left):
    a, b, c = parts
    return jnp.concatenate([a, b, c, a, b, a] if left else [a, a, a, b, b, c], axis=0)


def contract(a, b, da, db, **kw):
    return lax.dot_general(a, b, (((da,), (db,)), ((), ())), preferred_element_type=F32, **kw)


def kernel(n_tm, n_mp, width, x_hbm, z_hbm, start_hbm, slide_hbm, table_hbm, win_hbm, wg_hbm, wv_hbm, wd_hbm, wo_hbm,
           out_ref, eps_ref, start_ref, slide_ref, x_ref, z_ref, table_ref, win_ref, wg_ref, wv_ref, wd_ref, wo_ref, load, hown, even, odd, wbuf, a_scr, f_scr, y_scr, dbuf, obuf, pbuf,
           coef, wsend, wrecv, dsend, drecv, psend, osend, precv, rsend, rrecv):
    prompts, _, lat, pos = x_hbm.shape
    units = wg_ref.shape[1]
    rank = lat + prompts
    share = pos // n_mp
    cuts = share // width
    pieces = prompts * cuts
    n_z = n_tm // 2
    tm, mp = lax.axis_index("tm"), lax.axis_index("mp")
    zi, yi = lax.div(tm, 2), lax.rem(tm, 2)
    twin = tm + 1 - 2 * yi
    mesh_id = pl.DeviceIdType.MESH
    cols = pl.ds(pl.multiple_of(mp * share, 128), share)

    pairs = [(start_hbm, start_ref), (slide_hbm, slide_ref), (win_hbm, win_ref), (table_hbm, table_ref), (wg_hbm, wg_ref), (wv_hbm, wv_ref), (wo_hbm, wo_ref),
             (wd_hbm, wd_ref), (x_hbm.at[:, :, :, cols], x_ref), (z_hbm.at[:, :, :, cols], z_ref)]
    loads = [pltpu.make_async_copy(a, b, load.at[i]) for i, (a, b) in enumerate(pairs)]
    for one in loads:
        one.start()
    barrier = pltpu.get_barrier_semaphore()

    def over_z(op):
        lax.fori_loop(0, n_z - 1, lambda k, c: (op(k, k + jnp.where(k >= zi, 1, 0)), c)[1], 0)

    def peer(k):
        at = mp
        for b in range(k.bit_length()):
            if k >> b & 1:
                at = at + (1 << b) * (1 - 2 * lax.rem(lax.div(mp, 1 << b), 2))
        return at

    def greet(device):
        pl.semaphore_signal(barrier, inc=1, device_id=device, device_id_type=mesh_id)

    over_z(lambda k, z: greet({"tm": 2 * z + yi}))
    for k in range(1, n_mp):
        greet({"mp": peer(k)})
    for k in range(0, n_mp, 2):
        greet({"tm": twin, "mp": peer(k)})

    for one in loads[:8]:
        one.wait()
    channels = win_ref.shape[1]
    order = lax.broadcasted_iota(jnp.int32, (prompts, channels), 0)
    times = jnp.zeros((prompts, channels), F32)
    for p in range(prompts):
        times = jnp.where(order == p, (start_ref[p] - tm).astype(F32), times)
    angle = times * table_ref[3:4, :channels]
    lane = lax.broadcasted_iota(jnp.int32, (prompts, channels), 1)
    emb = jnp.where(lane < channels // 2, jnp.cos(angle), jnp.sin(angle))
    raw = jnp.concatenate([win_ref[...], emb], axis=0)
    left = raw - jnp.mean(raw, axis=1, keepdims=True)
    l3 = jnp.concatenate(split3(left), axis=0).astype(BF16)

    def folded(weights, width, db):
        got = contract(l3 if db == 0 else o3, weights, 1, db)
        return got[:width] + got[width:2 * width] + got[2 * width:3 * width]

    wot = wo_ref[...]
    o3 = jnp.concatenate(split3(wot) + (jnp.zeros_like(wot),), axis=0).astype(BF16)
    root = math.sqrt(0.5)
    wbuf[0, 0:rank] = folded(wg_ref[...], rank, 0) * root
    wbuf[0, rank:2 * rank] = folded(wv_ref[...], rank, 0) * root
    wbuf[0, 2 * rank:2 * rank + lat] = folded(wd_ref[...], lat, 1)

    def build(k):
        for part in range(2):
            a, b, c = split3(wbuf[k, part * rank:(part + 1) * rank])
            a_scr[k, part * units:(part + 1) * units] = six((a, b, c), True).T.astype(BF16)
        a, b, c = split3(wbuf[k, 2 * rank:2 * rank + lat])
        f_scr[:, k * units:(k + 1) * units] = jnp.concatenate([a, b, c, jnp.zeros_like(a)], axis=0).astype(BF16)

    grid = lax.broadcasted_iota(jnp.int32, table_ref.shape, 1)
    for p in range(prompts):
        picked = jnp.where(grid == start_ref[p] - tm, table_ref[...], 0.0)
        coef[p] = jnp.broadcast_to(jnp.sum(picked, axis=1, keepdims=True), coef.shape[1:])

    base = contract(raw, wot, 1, 1, precision=HIGH)
    base6 = six(split3(base), True).T.astype(BF16)
    gram = contract(left, left, 1, 1, precision=HIGH) * (1.0 / channels)
    gram6 = six(split3(gram), True).T.astype(BF16)
    rows = lax.broadcasted_iota(jnp.int32, (prompts, share), 0)
    for one in loads[8:]:
        one.wait()
    for p in range(prompts):
        u = jnp.concatenate([x_ref[p, 0], (rows == p).astype(F32)], axis=0)
        u6 = six(split3(u), False).astype(BF16)
        gu = jnp.dot(gram6, u6, preferred_element_type=F32)
        eps_ref[p, 0] = jnp.dot(base6, u6, preferred_element_type=F32)
        var = jnp.maximum(jnp.sum(gu * u, axis=0, keepdims=True), 0.0)
        y_scr[p] = six(split3(u * lax.rsqrt(var + 1e-5)), False).astype(BF16)

    def split(q):
        return lax.div(q, cuts), pl.ds(pl.multiple_of(lax.rem(q, cuts) * width, 128), width)

    def gated(k, yt):
        gate = jnp.dot(a_scr[k, :units], yt, preferred_element_type=F32)
        value = jnp.dot(a_scr[k, units:], yt, preferred_element_type=F32)
        return ((gate * (1.0 + lax.erf(gate))) * value).astype(BF16)

    def early(q, k):
        p, at = split(q)
        hown[q, k * units:(k + 1) * units] = gated(k, y_scr[p, :, at])

    def sweep(q, hid):
        p, at = split(q)
        yt = y_scr[p, :, at]
        for k in range(2, n_mp):
            hid[(k - 2) * units:(k - 1) * units] = gated(k, yt)

    def drift_copy(q, k, z):
        return pltpu.make_async_remote_copy(
            dbuf.at[zi, q], dbuf.at[zi, q], dsend.at[k, q], drecv.at[zi, q],
            device_id={"tm": 2 * z + yi}, device_id_type=mesh_id)

    def drift_arrival(q, k, z):
        return pltpu.make_async_remote_copy(
            dbuf.at[z, q], dbuf.at[z, q], dsend.at[k, q], drecv.at[z, q],
            device_id={"tm": 2 * z + yi}, device_id_type=mesh_id)

    def step(q, hid):
        p, at = split(q)
        got = jnp.dot(f_scr[...], jnp.concatenate([hown[q], hid[...]], axis=0), preferred_element_type=F32)
        eps = eps_ref[p, 0, :, at] + got[:lat] + got[lat:2 * lat] + got[2 * lat:3 * lat]
        eps_ref[p, 0, :, at] = eps
        x = x_ref[p, 0, :, at]
        c = coef[p]
        term = c[0:1, :1] * x - c[1:2, :1] * eps + c[2:3, :1] * z_ref[p, 0, :, at]
        dbuf[zi, q] = term + jnp.where(tm == 0, 1.0, 0.0) * x
        over_z(lambda k, z: drift_copy(q, k, z).start())

    def place(q, owner):
        return pl.ds(pl.multiple_of(owner * share + lax.rem(q, cuts) * width, 128), width)

    def own_copy(q, k):
        spot = pbuf.at[yi, lax.div(q, cuts), :, place(q, mp)]
        return pltpu.make_async_remote_copy(
            spot, spot, psend.at[k, q], precv.at[yi, mp, q],
            device_id={"mp": peer(k)}, device_id_type=mesh_id)

    def twin_copy(q, k):
        spot = pbuf.at[yi, lax.div(q, cuts), :, place(q, mp)]
        return pltpu.make_async_remote_copy(
            obuf.at[q], spot, osend.at[k, q], precv.at[yi, mp, q],
            device_id={"tm": twin, "mp": peer(k)}, device_id_type=mesh_id)

    def arrival(q, side, k):
        spot = pbuf.at[side, lax.div(q, cuts), :, place(q, peer(k))]
        return pltpu.make_async_remote_copy(
            spot, spot, psend.at[k, q], precv.at[side, peer(k), q],
            device_id={"mp": peer(1)}, device_id_type=mesh_id)

    def finish(q):
        over_z(lambda k, z: drift_arrival(q, k, z).wait_recv())
        p = lax.div(q, cuts)
        mine = jnp.minimum(tm + slide_ref[p], n_tm - 1)
        theirs = jnp.minimum(twin + slide_ref[p], n_tm - 1)

        def add(z, totals):
            part = dbuf[z, q]
            slot = 2 * z + yi
            return (totals[0] + jnp.where(slot < mine, 1.0, 0.0) * part,
                    totals[1] + jnp.where(slot < theirs, 1.0, 0.0) * part)

        zero = jnp.zeros((lat, width), F32)
        keep, give = lax.fori_loop(0, n_z, add, (zero, zero), unroll=n_z <= 8)
        pbuf[yi, p, :, place(q, mp)] = keep
        obuf[q] = give
        for k in range(0, n_mp, 2):
            twin_copy(q, k).start()
        for k in range(2, n_mp, 2):
            own_copy(q, k).start()

    def relay_copy(q, k, owner):
        spot = out_ref.at[lax.div(q, cuts), 0, :, place(q, owner)]
        return pltpu.make_async_remote_copy(
            spot, spot, rsend.at[k, q], rrecv.at[k, q], device_id={"mp": peer(1)}, device_id_type=mesh_id)

    def relay(q):
        p = lax.div(q, cuts)
        for k in range(0, n_mp, 2):
            arrival(q, 1 - yi, k).wait_recv()
            if k:
                arrival(q, yi, k).wait_recv()
            at = place(q, peer(k))
            out_ref[p, 0, :, at] = pbuf[0, p, :, at] + pbuf[1, p, :, at]
            relay_copy(q, k, peer(k)).start()

    def loop(count, op, start=0):
        lax.fori_loop(start, count, lambda q, c: (op(q), c)[1], 0)

    def table_copy(k):
        return pltpu.make_async_remote_copy(
            wbuf.at[0], wbuf.at[k], wsend.at[k], wrecv.at[k], device_id={"mp": peer(k)}, device_id_type=mesh_id)

    build(0)
    @pl.when(zi == 0)
    def _():
        loop(pieces, lambda q: early(q, 0))

    pl.semaphore_wait(barrier, n_z - 1 + n_mp - 1 + n_mp // 2)
    for k in range(1, n_mp):
        table_copy(k).start()

    @pl.when(zi != 0)
    def _():
        for q in range(pieces):
            early(q, 0)

    table_copy(1).wait_recv()
    build(1)
    for q in range(pieces):
        early(q, 1)
    for k in range(2, n_mp):
        table_copy(k).wait_recv()
        build(k)

    def lap(i):
        sweep(2 * i + 1, odd)
        step(2 * i, even)
        sweep(2 * i + 2, even)
        step(2 * i + 1, odd)

    sweep(0, even)
    loop(pieces // 2 - 1, lap)
    sweep(pieces - 1, odd)
    step(pieces - 2, even)
    step(pieces - 1, odd)
    loop(pieces, finish)
    loop(pieces, relay)

    def settle(q):
        for k in range(0, n_mp, 2):
            relay_copy(q, k, peer(k + 1)).wait_recv()

    loop(pieces, settle)
    for k in range(1, n_mp):
        table_copy(k).wait_send()

    def drain(q):
        over_z(lambda k, z: drift_copy(q, k, z).wait_send())
        for k in range(0, n_mp, 2):
            twin_copy(q, k).wait_send()
            relay_copy(q, k, peer(k)).wait_send()
        for k in range(2, n_mp, 2):
            own_copy(q, k).wait_send()

    loop(pieces, drain)


def shards(n_tm, n_mp, latents, noise, start_step, slide, w_in, w_gate, w_value, w_down, w_out):
    prompts, t_dev, lat, pos = latents.shape
    channels, units = w_gate.shape
    share = pos // n_mp
    rank = lat + prompts
    width = 512
    pieces = prompts * share // width
    n_z = n_tm // 2
    assert t_dev == 1 and n_tm % 2 == 0 and pieces % 2 == 0 and n_mp > 2 and n_mp & (n_mp - 1) == 0
    vmem = pl.BlockSpec(memory_space=pltpu.VMEM)
    dma = pltpu.SemaphoreType.DMA
    hbm = pl.BlockSpec(memory_space=pltpu.HBM)
    table = step_table(channels)
    return pl.pallas_call(
        functools.partial(kernel, n_tm, n_mp, width),
        out_shape=(pltpu.VMEM(latents.shape, F32), pltpu.VMEM((prompts, 1, lat, share), F32)),
        in_specs=[hbm] * 10,
        out_specs=(vmem, vmem),
        scratch_shapes=[
            pltpu.SMEM(start_step.shape, jnp.int32),
            pltpu.SMEM(slide.shape, jnp.int32),
            pltpu.VMEM((prompts, 1, lat, share), F32),
            pltpu.VMEM((prompts, 1, lat, share), F32),
            pltpu.VMEM(table.shape, F32),
            pltpu.VMEM(w_in.shape, F32),
            pltpu.VMEM(w_gate.shape, BF16),
            pltpu.VMEM(w_value.shape, BF16),
            pltpu.VMEM(w_down.shape, BF16),
            pltpu.VMEM(w_in.shape, F32),
            dma((10,)),
            pltpu.VMEM((pieces, 2 * units, width), BF16),
            pltpu.VMEM((n_mp * units - 2 * units, width), BF16),
            pltpu.VMEM((n_mp * units - 2 * units, width), BF16),
            pltpu.VMEM((n_mp, 2 * rank + 8, units), F32),
            pltpu.VMEM((n_mp, 2 * units, 6 * rank), BF16),
            pltpu.VMEM((4 * lat, n_mp * units), BF16),
            pltpu.VMEM((prompts, 6 * rank, share), BF16),
            pltpu.VMEM((n_z, pieces, lat, width), F32),
            pltpu.VMEM((pieces, lat, width), F32),
            pltpu.VMEM((2, prompts, lat, pos), F32),
            pltpu.VMEM((prompts, 4, 128), F32),
            dma((n_mp,)), dma((n_mp,)),
            dma((n_z, pieces)), dma((n_z, pieces)),
            dma((n_mp, pieces)), dma((n_mp, pieces)), dma((2, n_mp, pieces)),
            dma((n_mp, pieces)), dma((n_mp, pieces)),
        ],
        compiler_params=pltpu.CompilerParams(collective_id=0, has_side_effects=True, vmem_limit_bytes=60000 * 1024),
    )(latents, noise, start_step, slide, table, w_in, w_gate, w_value, w_down, w_out.T)


def solution(mesh):
    in_specs = (
        P(None, "tm", None, None),
        P(None, "tm", None, None),
        P(),
        P(),
        P(),
        P(None, "mp"),
        P(None, "mp"),
        P("mp", None),
        P(),
    )
    out_specs = (P(None, "tm", None, None), P(None, "tm", None, "mp"))
    body = functools.partial(shards, mesh.shape["tm"], mesh.shape["mp"])
    return jax.shard_map(body, mesh=mesh, in_specs=in_specs, out_specs=out_specs, check_vma=False)
```

```python
import functools
import math

import jax
import jax.numpy as jnp
import numpy as np
from jax import lax
from jax.experimental import pallas as pl
from jax.experimental.pallas import tpu as pltpu
from jax.sharding import PartitionSpec as P

TSTEPS = 1000
F32, BF16 = jnp.float32, jnp.bfloat16
HIGH = lax.Precision.HIGHEST


def step_table(channels):
    beta = 1e-4 + (0.02 - 1e-4) * np.arange(TSTEPS, dtype=np.float64) / (TSTEPS - 1)
    abar = np.cumprod(1.0 - beta)
    root = np.sqrt(1.0 - beta)
    half = channels // 2
    freq = np.exp(-math.log(10000.0) * np.arange(half, dtype=np.float64) / half)
    table = np.zeros((4, max(TSTEPS, channels)), np.float32)
    table[:3, :TSTEPS] = [1.0 / root - 1.0, beta / np.sqrt(1.0 - abar) / root, np.sqrt(beta)]
    table[3, :channels] = np.concatenate([freq, freq])
    return table


def split3(v):
    a = v.astype(BF16).astype(F32)
    rest = v - a
    b = rest.astype(BF16).astype(F32)
    return a, b, rest - b


def six(parts, left):
    a, b, c = parts
    return jnp.concatenate([a, b, c, a, b, a] if left else [a, a, a, b, b, c], axis=0)


def contract(a, b, da, db, **kw):
    return lax.dot_general(a, b, (((da,), (db,)), ((), ())), preferred_element_type=F32, **kw)


def kernel(n_tm, n_mp, width, x_hbm, z_hbm, start_hbm, slide_hbm, table_hbm, win_hbm, wg_hbm, wv_hbm, wd_hbm, wo_hbm,
           out_ref, eps_ref, plan_ref, xz_ref, table_ref, io_ref, w_ref, load, hown, even, odd, wbuf, a_scr, f_scr, y_scr, dbuf, obuf, pbuf,
           coef, wsend, wrecv, dsend, drecv, psend, precv, rsend, rrecv):
    prompts, _, lat, pos = x_hbm.shape
    units = w_ref.shape[2]
    rank = lat + prompts
    share = pos // n_mp
    cuts = share // width
    pieces = prompts * cuts
    n_z = n_tm // 2
    tm, mp = lax.axis_index("tm"), lax.axis_index("mp")
    zi, yi = lax.div(tm, 2), lax.rem(tm, 2)
    twin = tm + 1 - 2 * yi
    mesh_id = pl.DeviceIdType.MESH
    cols = pl.ds(pl.multiple_of(mp * share, 128), share)

    groups = [[(start_hbm, plan_ref.at[0]), (slide_hbm, plan_ref.at[1])],
              [(table_hbm, table_ref)],
              [(win_hbm, io_ref.at[0]), (wo_hbm, io_ref.at[1])],
              [(wg_hbm, w_ref.at[0]), (wv_hbm, w_ref.at[1]), (wd_hbm, w_ref.at[2])],
              [(x_hbm.at[:, :, :, cols], xz_ref.at[0]), (z_hbm.at[:, :, :, cols], xz_ref.at[1])]]
    for i, group in enumerate(groups):
        for a, b in group:
            pltpu.make_async_copy(a, b, load.at[i]).start()
    whole = [pltpu.make_async_copy(a, a, load.at[i]) for i, a in enumerate((plan_ref, table_ref, io_ref, w_ref, xz_ref))]
    barrier = pltpu.get_barrier_semaphore()

    def over_z(op):
        lax.fori_loop(0, n_z - 1, lambda k, c: (op(k, k + jnp.where(k >= zi, 1, 0)), c)[1], 0)

    def peer(k):
        at = mp
        for b in range(k.bit_length()):
            if k >> b & 1:
                at = at + (1 << b) * (1 - 2 * lax.rem(lax.div(mp, 1 << b), 2))
        return at

    def greet(device):
        pl.semaphore_signal(barrier, inc=1, device_id=device, device_id_type=mesh_id)

    over_z(lambda k, z: greet({"tm": 2 * z + yi}))
    for k in range(1, n_mp):
        greet({"mp": peer(k)})
    for k in range(0, n_mp, 2):
        greet({"tm": twin, "mp": peer(k)})

    for one in whole[:4]:
        one.wait()
    channels = io_ref.shape[2]
    order = lax.broadcasted_iota(jnp.int32, (prompts, channels), 0)
    times = jnp.zeros((prompts, channels), F32)
    for p in range(prompts):
        times = jnp.where(order == p, (plan_ref[0, p] - tm).astype(F32), times)
    angle = times * table_ref[3:4, :channels]
    lane = lax.broadcasted_iota(jnp.int32, (prompts, channels), 1)
    emb = jnp.where(lane < channels // 2, jnp.cos(angle), jnp.sin(angle))
    raw = jnp.concatenate([io_ref[0], emb], axis=0)
    left = raw - jnp.mean(raw, axis=1, keepdims=True)
    l3 = jnp.concatenate(split3(left), axis=0).astype(BF16)

    def folded(weights, width, db):
        got = contract(l3 if db == 0 else o3, weights, 1, db)
        return got[:width] + got[width:2 * width] + got[2 * width:3 * width]

    wot = io_ref[1]
    o3 = jnp.concatenate(split3(wot) + (jnp.zeros_like(wot),), axis=0).astype(BF16)
    root = math.sqrt(0.5)
    wbuf[0, 0:rank] = folded(w_ref[0], rank, 0) * root
    wbuf[0, rank:2 * rank] = folded(w_ref[1], rank, 0) * root
    wbuf[0, 2 * rank:2 * rank + lat] = folded(w_ref[2], lat, 1)

    def build(k):
        for part in range(2):
            a, b, c = split3(wbuf[k, part * rank:(part + 1) * rank])
            a_scr[k, part * units:(part + 1) * units] = six((a, b, c), True).T.astype(BF16)
        a, b, c = split3(wbuf[k, 2 * rank:2 * rank + lat])
        f_scr[:, k * units:(k + 1) * units] = jnp.concatenate([a, b, c, jnp.zeros_like(a)], axis=0).astype(BF16)

    grid = lax.broadcasted_iota(jnp.int32, table_ref.shape, 1)
    for p in range(prompts):
        picked = jnp.where(grid == plan_ref[0, p] - tm, table_ref[...], 0.0)
        coef[p] = jnp.broadcast_to(jnp.sum(picked, axis=1, keepdims=True), coef.shape[1:])

    base = contract(raw, wot, 1, 1, precision=HIGH)
    base6 = six(split3(base), True).T.astype(BF16)
    gram = contract(left, left, 1, 1, precision=HIGH) * (1.0 / channels)
    gram6 = six(split3(gram), True).T.astype(BF16)
    rows = lax.broadcasted_iota(jnp.int32, (prompts, share), 0)
    whole[4].wait()
    for p in range(prompts):
        u = jnp.concatenate([xz_ref[0, p, 0], (rows == p).astype(F32)], axis=0)
        u6 = six(split3(u), False).astype(BF16)
        gu = jnp.dot(gram6, u6, preferred_element_type=F32)
        eps_ref[p, 0] = jnp.dot(base6, u6, preferred_element_type=F32)
        var = jnp.maximum(jnp.sum(gu * u, axis=0, keepdims=True), 0.0)
        y_scr[p] = six(split3(u * lax.rsqrt(var + 1e-5)), False).astype(BF16)

    def split(q):
        return lax.div(q, cuts), pl.ds(pl.multiple_of(lax.rem(q, cuts) * width, 128), width)

    def gated(k, yt):
        gate = jnp.dot(a_scr[k, :units], yt, preferred_element_type=F32)
        value = jnp.dot(a_scr[k, units:], yt, preferred_element_type=F32)
        return ((gate * (1.0 + lax.erf(gate))) * value).astype(BF16)

    def early(q, k):
        p, at = split(q)
        hown[q, k * units:(k + 1) * units] = gated(k, y_scr[p, :, at])

    def sweep(q, hid):
        p, at = split(q)
        yt = y_scr[p, :, at]
        for k in range(2, n_mp):
            hid[(k - 2) * units:(k - 1) * units] = gated(k, yt)

    def remote(src, dst, send, recv, device):
        return pltpu.make_async_remote_copy(src, dst, send, recv, device_id=device, device_id_type=mesh_id)

    def bulk(ref, sem):
        return remote(ref, ref, sem, sem, {"mp": peer(1)})

    def drift_copy(q, z):
        return remote(dbuf.at[q, zi], dbuf.at[q, zi], dsend.at[0], drecv.at[q], {"tm": 2 * z + yi})

    def step(q, hid):
        p, at = split(q)
        got = jnp.dot(f_scr[...], jnp.concatenate([hown[q], hid[...]], axis=0), preferred_element_type=F32)
        eps = eps_ref[p, 0, :, at] + got[:lat] + got[lat:2 * lat] + got[2 * lat:3 * lat]
        eps_ref[p, 0, :, at] = eps
        x = xz_ref[0, p, 0, :, at]
        c = coef[p]
        term = c[0:1, :1] * x - c[1:2, :1] * eps + c[2:3, :1] * xz_ref[1, p, 0, :, at]
        dbuf[q, zi] = term + jnp.where(tm == 0, 1.0, 0.0) * x
        over_z(lambda k, z: drift_copy(q, z).start())

    def place(q, owner):
        return pl.ds(pl.multiple_of(owner * share + lax.rem(q, cuts) * width, 128), width)

    def own_copy(q, k):
        spot = pbuf.at[q, yi, mp]
        return remote(spot, spot, psend.at[0], precv.at[q], {"mp": peer(k)})

    def twin_copy(q, k):
        return remote(obuf.at[q], pbuf.at[q, yi, mp], psend.at[0], precv.at[q], {"tm": twin, "mp": peer(k)})

    def finish(q):
        bulk(dbuf.at[q, pl.ds(0, n_z - 1)], drecv.at[q]).wait_recv()
        p = lax.div(q, cuts)
        mine = jnp.minimum(tm + plan_ref[1, p], n_tm - 1)
        theirs = jnp.minimum(twin + plan_ref[1, p], n_tm - 1)

        def add(z, totals):
            part = dbuf[q, z]
            slot = 2 * z + yi
            return (totals[0] + jnp.where(slot < mine, 1.0, 0.0) * part,
                    totals[1] + jnp.where(slot < theirs, 1.0, 0.0) * part)

        zero = jnp.zeros((lat, width), F32)
        keep, give = lax.fori_loop(0, n_z, add, (zero, zero), unroll=n_z <= 8)
        pbuf[q, yi, mp] = keep
        obuf[q] = give
        for k in range(0, n_mp, 2):
            twin_copy(q, k).start()
        for k in range(2, n_mp, 2):
            own_copy(q, k).start()

    def relay(q):
        p = lax.div(q, cuts)
        bulk(pbuf.at[q, 0, pl.ds(0, n_mp - 1)], precv.at[q]).wait_recv()
        for k in range(0, n_mp, 2):
            owner = peer(k)
            at = place(q, owner)
            out_ref[p, 0, :, at] = pbuf[q, 0, owner] + pbuf[q, 1, owner]
            spot = out_ref.at[p, 0, :, at]
            remote(spot, spot, rsend.at[0], rrecv.at[0], {"mp": peer(1)}).start()

    def loop(count, op, start=0):
        lax.fori_loop(start, count, lambda q, c: (op(q), c)[1], 0)

    def table_copy(k):
        return remote(wbuf.at[0], wbuf.at[k], wsend.at[0], wrecv.at[min(k, 2) - 1], {"mp": peer(k)})

    build(0)
    @pl.when(zi == 0)
    def _():
        loop(pieces, lambda q: early(q, 0))

    pl.semaphore_wait(barrier, n_z - 1 + n_mp - 1 + n_mp // 2)
    for k in range(1, n_mp):
        table_copy(k).start()

    @pl.when(zi != 0)
    def _():
        for q in range(pieces):
            early(q, 0)

    bulk(wbuf.at[1], wrecv.at[0]).wait_recv()
    build(1)
    for q in range(pieces):
        early(q, 1)
    bulk(wbuf.at[pl.ds(2, n_mp - 2)], wrecv.at[1]).wait_recv()
    for k in range(2, n_mp):
        build(k)

    def lap(i):
        sweep(2 * i + 1, odd)
        step(2 * i, even)
        sweep(2 * i + 2, even)
        step(2 * i + 1, odd)

    sweep(0, even)
    loop(pieces // 2 - 1, lap)
    sweep(pieces - 1, odd)
    step(pieces - 2, even)
    step(pieces - 1, odd)
    loop(pieces, finish)
    loop(pieces, relay)

    half = out_ref.at[:, :, :, pl.ds(0, pos // 2)]
    bulk(half, rrecv.at[0]).wait_recv()
    bulk(half, rsend.at[0]).wait_send()
    bulk(wbuf.at[pl.ds(1, n_mp - 1)], wsend.at[0]).wait_send()
    bulk(dbuf.at[:, pl.ds(0, n_z - 1)], dsend.at[0]).wait_send()
    bulk(pbuf.at[:, 0, pl.ds(0, n_mp - 1)], psend.at[0]).wait_send()


def shards(n_tm, n_mp, latents, noise, start_step, slide, w_in, w_gate, w_value, w_down, w_out):
    prompts, t_dev, lat, pos = latents.shape
    channels, units = w_gate.shape
    share = pos // n_mp
    rank = lat + prompts
    width = 512
    pieces = prompts * share // width
    n_z = n_tm // 2
    assert w_gate.shape == w_down.shape and t_dev == 1 and n_tm % 2 == 0 and pieces % 2 == 0 and n_mp > 2 and n_mp & (n_mp - 1) == 0
    vmem = pl.BlockSpec(memory_space=pltpu.VMEM)
    dma = pltpu.SemaphoreType.DMA
    hbm = pl.BlockSpec(memory_space=pltpu.HBM)
    table = step_table(channels)
    return pl.pallas_call(
        functools.partial(kernel, n_tm, n_mp, width),
        out_shape=(pltpu.VMEM(latents.shape, F32), pltpu.VMEM((prompts, 1, lat, share), F32)),
        in_specs=[hbm] * 10,
        out_specs=(vmem, vmem),
        scratch_shapes=[
            pltpu.SMEM((2, prompts), jnp.int32),
            pltpu.VMEM((2, prompts, 1, lat, share), F32),
            pltpu.VMEM(table.shape, F32),
            pltpu.VMEM((2,) + w_in.shape, F32),
            pltpu.VMEM((3,) + w_gate.shape, BF16),
            dma((5,)),
            pltpu.VMEM((pieces, 2 * units, width), BF16),
            pltpu.VMEM((n_mp * units - 2 * units, width), BF16),
            pltpu.VMEM((n_mp * units - 2 * units, width), BF16),
            pltpu.VMEM((n_mp, 2 * rank + 8, units), F32),
            pltpu.VMEM((n_mp, 2 * units, 6 * rank), BF16),
            pltpu.VMEM((4 * lat, n_mp * units), BF16),
            pltpu.VMEM((prompts, 6 * rank, share), BF16),
            pltpu.VMEM((pieces, n_z, lat, width), F32),
            pltpu.VMEM((pieces, lat, width), F32),
            pltpu.VMEM((pieces, 2, n_mp, lat, width), F32),
            pltpu.VMEM((prompts, 4, 128), F32),
            dma((1,)), dma((2,)),
            dma((1,)), dma((pieces,)),
            dma((1,)), dma((pieces,)),
            dma((1,)), dma((1,)),
        ],
        compiler_params=pltpu.CompilerParams(collective_id=0, has_side_effects=True, vmem_limit_bytes=60000 * 1024),
    )(latents, noise, start_step, slide, table, w_in, w_gate, w_value, w_down, w_out.T)


def solution(mesh):
    in_specs = (
        P(None, "tm", None, None),
        P(None, "tm", None, None),
        P(),
        P(),
        P(),
        P(None, "mp"),
        P(None, "mp"),
        P("mp", None),
        P(),
    )
    out_specs = (P(None, "tm", None, None), P(None, "tm", None, "mp"))
    body = functools.partial(shards, mesh.shape["tm"], mesh.shape["mp"])
    return jax.shard_map(body, mesh=mesh, in_specs=in_specs, out_specs=out_specs, check_vma=False)
```

```python
import functools
import math

import jax
import jax.numpy as jnp
import numpy as np
from jax import lax
from jax.experimental import pallas as pl
from jax.experimental.pallas import tpu as pltpu
from jax.sharding import PartitionSpec as P

TSTEPS = 1000
DIRECT = 2
F32, BF16 = jnp.float32, jnp.bfloat16
HIGH = lax.Precision.HIGHEST


def step_table(channels):
    beta = 1e-4 + (0.02 - 1e-4) * np.arange(TSTEPS, dtype=np.float64) / (TSTEPS - 1)
    abar = np.cumprod(1.0 - beta)
    root = np.sqrt(1.0 - beta)
    half = channels // 2
    freq = np.exp(-math.log(10000.0) * np.arange(half, dtype=np.float64) / half)
    table = np.zeros((4, max(TSTEPS, channels)), np.float32)
    table[:3, :TSTEPS] = [1.0 / root - 1.0, beta / np.sqrt(1.0 - abar) / root, np.sqrt(beta)]
    table[3, :channels] = np.concatenate([freq, freq])
    return table


def split3(v):
    a = v.astype(BF16).astype(F32)
    rest = v - a
    b = rest.astype(BF16).astype(F32)
    return a, b, rest - b


def six(parts, left):
    a, b, c = parts
    return jnp.concatenate([a, b, c, a, b, a] if left else [a, a, a, b, b, c], axis=0)


def contract(a, b, da, db, **kw):
    return lax.dot_general(a, b, (((da,), (db,)), ((), ())), preferred_element_type=F32, **kw)


def kernel(n_tm, n_mp, width, x_hbm, z_hbm, start_hbm, slide_hbm, table_hbm, win_hbm, wg_hbm, wv_hbm, wd_hbm, wo_hbm,
           out_ref, eps_ref, plan_ref, xz_ref, table_ref, io_ref, w_ref, load, hown, even, odd, wbuf, fbuf, a_scr, f_scr, y_scr, dbuf, obuf, pbuf,
           coef, wsend, wrecv, dsend, drecv, psend, precv, rsend, rrecv, zsem):
    prompts, _, lat, pos = x_hbm.shape
    units = w_ref.shape[2]
    rank = lat + prompts
    share = pos // n_mp
    cuts = share // width
    pieces = prompts * cuts
    n_z = n_tm // 2
    tm, mp = lax.axis_index("tm"), lax.axis_index("mp")
    zi, yi = lax.div(tm, 2), lax.rem(tm, 2)
    twin = tm + 1 - 2 * yi
    mesh_id = pl.DeviceIdType.MESH
    cols = pl.ds(pl.multiple_of(mp * share, 128), share)

    groups = [[(start_hbm, plan_ref.at[0]), (slide_hbm, plan_ref.at[1])],
              [(table_hbm, table_ref)],
              [(win_hbm, io_ref.at[0]), (wo_hbm, io_ref.at[1])],
              [(wg_hbm, w_ref.at[0]), (wv_hbm, w_ref.at[1]), (wd_hbm, w_ref.at[2])],
              [(x_hbm.at[:, :, :, cols], xz_ref.at[0]), (z_hbm.at[:, :, :, cols], xz_ref.at[1])]]
    for i, group in enumerate(groups):
        for a, b in group:
            pltpu.make_async_copy(a, b, load.at[i]).start()
    whole = [pltpu.make_async_copy(a, a, load.at[i]) for i, a in enumerate((plan_ref, table_ref, io_ref, w_ref, xz_ref))]
    barrier = pltpu.get_barrier_semaphore()

    def peer(k):
        at = mp
        for b in range(k.bit_length()):
            if k >> b & 1:
                at = at + (1 << b) * (1 - 2 * lax.rem(lax.div(mp, 1 << b), 2))
        return at

    def greet(device):
        pl.semaphore_signal(barrier, inc=1, device_id=device, device_id_type=mesh_id)

    lax.fori_loop(zi + 1, n_z, lambda z, c: (greet({"tm": 2 * z + yi}), c)[1], 0)
    for k in range(1, n_mp):
        greet({"mp": peer(k)})
    for k in range(n_mp):
        greet({"tm": twin, "mp": peer(k)})

    for one in whole[:3]:
        one.wait()
    channels = io_ref.shape[2]
    order = lax.broadcasted_iota(jnp.int32, (prompts, channels), 0)
    times = jnp.zeros((prompts, channels), F32)
    for p in range(prompts):
        times = jnp.where(order == p, (plan_ref[0, p] - tm).astype(F32), times)
    angle = times * table_ref[3:4, :channels]
    lane = lax.broadcasted_iota(jnp.int32, (prompts, channels), 1)
    emb = jnp.where(lane < channels // 2, jnp.cos(angle), jnp.sin(angle))
    raw = jnp.concatenate([io_ref[0], emb], axis=0)
    left = raw - jnp.mean(raw, axis=1, keepdims=True)
    l3 = jnp.concatenate(split3(left), axis=0).astype(BF16)

    def folded(weights, width, db):
        got = contract(l3 if db == 0 else o3, weights, 1, db)
        return got[:width] + got[width:2 * width] + got[2 * width:3 * width]

    wot = io_ref[1]
    o3 = jnp.concatenate(split3(wot) + (jnp.zeros_like(wot),), axis=0).astype(BF16)
    root = math.sqrt(0.5)
    whole[3].wait()
    wbuf[0, 0:rank] = folded(w_ref[0], rank, 0) * root
    wbuf[0, rank:2 * rank] = folded(w_ref[1], rank, 0) * root
    fbuf[0] = folded(w_ref[2], lat, 1)

    def build(k):
        for part in range(2):
            a, b, c = split3(wbuf[k, part * rank:(part + 1) * rank])
            a_scr[k, part * units:(part + 1) * units] = six((a, b, c), True).T.astype(BF16)

    def build_down(k):
        a, b, c = split3(fbuf[k])
        f_scr[:, k * units:(k + 1) * units] = jnp.concatenate([a, b, c, jnp.zeros_like(a)], axis=0).astype(BF16)

    grid = lax.broadcasted_iota(jnp.int32, table_ref.shape, 1)
    for p in range(prompts):
        picked = jnp.where(grid == plan_ref[0, p] - tm, table_ref[...], 0.0)
        coef[p] = jnp.broadcast_to(jnp.sum(picked, axis=1, keepdims=True), coef.shape[1:])

    base = contract(raw, wot, 1, 1, precision=HIGH)
    base6 = six(split3(base), True).T.astype(BF16)
    gram = contract(left, left, 1, 1, precision=HIGH) * (1.0 / channels)
    gram6 = six(split3(gram), True).T.astype(BF16)
    rows = lax.broadcasted_iota(jnp.int32, (prompts, share), 0)
    whole[4].wait()
    for p in range(prompts):
        u = jnp.concatenate([xz_ref[0, p, 0], (rows == p).astype(F32)], axis=0)
        u6 = six(split3(u), False).astype(BF16)
        gu = jnp.dot(gram6, u6, preferred_element_type=F32)
        eps_ref[p, 0] = jnp.dot(base6, u6, preferred_element_type=F32)
        var = jnp.maximum(jnp.sum(gu * u, axis=0, keepdims=True), 0.0)
        y_scr[p] = six(split3(u * lax.rsqrt(var + 1e-5)), False).astype(BF16)

    def split(q):
        return lax.div(q, cuts), pl.ds(pl.multiple_of(lax.rem(q, cuts) * width, 128), width)

    def gated(k, yt):
        gate = jnp.dot(a_scr[k, :units], yt, preferred_element_type=F32)
        value = jnp.dot(a_scr[k, units:], yt, preferred_element_type=F32)
        return ((gate * (1.0 + lax.erf(gate))) * value).astype(BF16)

    def early(q, k):
        p, at = split(q)
        hown[q, k * units:(k + 1) * units] = gated(k, y_scr[p, :, at])

    def sweep(q, hid):
        p, at = split(q)
        yt = y_scr[p, :, at]
        for k in range(2, n_mp):
            hid[(k - 2) * units:(k - 1) * units] = gated(k, yt)

    def remote(src, dst, send, recv, device):
        return pltpu.make_async_remote_copy(src, dst, send, recv, device_id=device, device_id_type=mesh_id)

    def bulk(ref, sem):
        return remote(ref, ref, sem, sem, {"mp": peer(1)})

    def drift_copy(q, z):
        return remote(dbuf.at[q, zi], dbuf.at[q, zi], dsend.at[0], drecv.at[q], {"tm": 2 * z + yi})

    def down(q, weights, hidden):
        p, at = split(q)
        got = jnp.dot(weights, hidden, preferred_element_type=F32)
        eps = eps_ref[p, 0, :, at] + got[:lat] + got[lat:2 * lat] + got[2 * lat:3 * lat]
        eps_ref[p, 0, :, at] = eps
        return eps

    def send(q, low, high):
        lax.fori_loop(low, high, lambda k, c: (drift_copy(q, k + jnp.where(k >= zi, 1, 0)).start(), c)[1], 0)

    def step(q, hid):
        p, at = split(q)
        eps = down(q, f_scr[...], jnp.concatenate([hown[q], hid[...]], axis=0))
        x = xz_ref[0, p, 0, :, at]
        c = coef[p]
        term = c[0:1, :1] * x - c[1:2, :1] * eps + c[2:3, :1] * xz_ref[1, p, 0, :, at]
        dbuf[q, zi] = term + jnp.where(tm == 0, 1.0, 0.0) * x
        if q == 0:
            @pl.when(zi < n_z - 1)
            def _():
                pl.semaphore_wait(zsem, n_z - 1 - zi)

        send(q, 0, jnp.where(tm == n_tm - 1, 0, n_z - 1))

    def place(q, owner):
        return pl.ds(pl.multiple_of(owner * share + lax.rem(q, cuts) * width, 128), width)

    def own_copy(q, k, sem=0):
        spot = pbuf.at[q, yi, mp]
        return remote(spot, spot, psend.at[sem], precv.at[q], {"mp": peer(k)})

    def twin_copy(q, k, sem=0, arrive=None):
        return remote(obuf.at[q], pbuf.at[q, yi, mp], psend.at[sem], precv.at[q if arrive is None else arrive], {"tm": twin, "mp": peer(k)})

    def merge(q):
        short = (yi == 1) & (zi < n_z - 1)

        @pl.when(short)
        def _():
            bulk(dbuf.at[q, pl.ds(0, n_z - 2)], drecv.at[q]).wait_recv()

        @pl.when(jnp.logical_not(short))
        def _():
            bulk(dbuf.at[q, pl.ds(0, n_z - 1)], drecv.at[q]).wait_recv()

        p = lax.div(q, cuts)
        mine = jnp.minimum(tm + plan_ref[1, p], n_tm - 1)
        theirs = jnp.minimum(twin + plan_ref[1, p], n_tm - 1)

        def add(z, totals):
            part = dbuf[q, z]
            slot = 2 * z + yi
            return (totals[0] + jnp.where(slot < mine, 1.0, 0.0) * part,
                    totals[1] + jnp.where(slot < theirs, 1.0, 0.0) * part)

        zero = jnp.zeros((lat, width), F32)
        sums = lax.fori_loop(0, n_z - 1, add, (zero, zero), unroll=n_z <= 8)
        keep, give = lax.fori_loop(n_z - 1, n_z - yi, add, sums)
        pbuf[q, yi, mp] = keep
        obuf[q] = give

    def finish(q):
        merge(q)
        for k in range(0, n_mp, 2):
            twin_copy(q, k).start()
        for k in range(2, n_mp, 2):
            own_copy(q, k).start()

    def finish_direct(q):
        merge(q)
        for k in range(n_mp):
            twin_copy(q, k, 2, q + DIRECT).start()
        for k in range(1, n_mp):
            own_copy(q, k, 1).start()

    def gather_direct(q):
        p = lax.div(q, cuts)
        bulk(pbuf.at[q, 0, pl.ds(0, n_mp - 1)], precv.at[q]).wait_recv()
        bulk(pbuf.at[q, 1], precv.at[q + DIRECT]).wait_recv()
        for owner in range(n_mp):
            out_ref[p, 0, :, place(q, owner)] = pbuf[q, 0, owner] + pbuf[q, 1, owner]

    def relay(q):
        p = lax.div(q, cuts)
        bulk(pbuf.at[q, 0, pl.ds(0, n_mp - 1)], precv.at[q]).wait_recv()
        for k in range(0, n_mp, 2):
            owner = peer(k)
            at = place(q, owner)
            out_ref[p, 0, :, at] = pbuf[q, 0, owner] + pbuf[q, 1, owner]
            spot = out_ref.at[p, 0, :, at]
            remote(spot, spot, rsend.at[0], rrecv.at[0], {"mp": peer(1)}).start()

    def loop(count, op, start=0):
        lax.fori_loop(start, count, lambda q, c: (op(q), c)[1], 0)

    def table_copy(k, ref, at):
        return remote(ref.at[0], ref.at[k], wsend.at[at], wrecv.at[2 * at + min(k, 2) - 1], {"mp": peer(k)})

    build(0)
    build_down(0)
    pl.semaphore_wait(barrier, zi + n_mp - 1 + n_mp)

    def reply(z, c):
        pl.semaphore_signal(zsem, inc=1, device_id={"tm": 2 * z + yi}, device_id_type=mesh_id)
        return c

    lax.fori_loop(0, zi, reply, 0)
    order_k = list(range(1, n_mp))
    for k in order_k:
        table_copy(k, wbuf, 0).start()
    for k in order_k:
        table_copy(k, fbuf, 1).start()

    for q in range(pieces):
        early(q, 0)

    bulk(wbuf.at[1], wrecv.at[0]).wait_recv()
    bulk(fbuf.at[1], wrecv.at[2]).wait_recv()
    build(1)
    build_down(1)
    for q in range(pieces):
        early(q, 1)
    bulk(wbuf.at[pl.ds(2, n_mp - 2)], wrecv.at[1]).wait_recv()
    for k in range(2, n_mp):
        build(k)
    bulk(fbuf.at[pl.ds(2, n_mp - 2)], wrecv.at[3]).wait_recv()
    for k in range(2, n_mp):
        build_down(k)

    def lap(i):
        sweep(2 * i + 1, odd)
        step(2 * i, even)
        sweep(2 * i + 2, even)
        step(2 * i + 1, odd)

    sweep(0, even)
    for i in range(pieces // 2 - 1):
        lap(i)
    sweep(pieces - 1, odd)
    step(pieces - 2, even)
    step(pieces - 1, odd)
    loop(pieces - DIRECT, finish)
    loop(pieces, finish_direct, pieces - DIRECT)
    loop(pieces - DIRECT, relay)
    loop(pieces, gather_direct, pieces - DIRECT)

    half = pbuf.at[pl.ds(0, pieces - DIRECT), 0, pl.ds(0, n_mp // 2)]
    bulk(half, rrecv.at[0]).wait_recv()
    bulk(half, rsend.at[0]).wait_send()
    bulk(wbuf.at[pl.ds(1, n_mp - 1)], wsend.at[0]).wait_send()
    bulk(fbuf.at[pl.ds(1, n_mp - 1)], wsend.at[1]).wait_send()

    @pl.when(tm != n_tm - 1)
    def _():
        bulk(dbuf.at[:, pl.ds(0, n_z - 1)], dsend.at[0]).wait_send()

    bulk(pbuf.at[pl.ds(0, pieces - DIRECT), 0, pl.ds(0, n_mp - 1)], psend.at[0]).wait_send()
    bulk(pbuf.at[pl.ds(0, DIRECT), 0, pl.ds(0, n_mp - 1)], psend.at[1]).wait_send()
    bulk(pbuf.at[pl.ds(0, DIRECT), 0], psend.at[2]).wait_send()


def shards(n_tm, n_mp, latents, noise, start_step, slide, w_in, w_gate, w_value, w_down, w_out):
    prompts, t_dev, lat, pos = latents.shape
    channels, units = w_gate.shape
    share = pos // n_mp
    rank = lat + prompts
    width = 512
    pieces = prompts * share // width
    n_z = n_tm // 2
    assert w_gate.shape == w_down.shape and t_dev == 1 and n_tm % 2 == 0 and pieces % 2 == 0 and n_mp > 2 and n_mp & (n_mp - 1) == 0
    vmem = pl.BlockSpec(memory_space=pltpu.VMEM)
    dma = pltpu.SemaphoreType.DMA
    hbm = pl.BlockSpec(memory_space=pltpu.HBM)
    table = step_table(channels)
    return pl.pallas_call(
        functools.partial(kernel, n_tm, n_mp, width),
        out_shape=(pltpu.VMEM(latents.shape, F32), pltpu.VMEM((prompts, 1, lat, share), F32)),
        in_specs=[hbm] * 10,
        out_specs=(vmem, vmem),
        scratch_shapes=[
            pltpu.SMEM((2, prompts), jnp.int32),
            pltpu.VMEM((2, prompts, 1, lat, share), F32),
            pltpu.VMEM(table.shape, F32),
            pltpu.VMEM((2,) + w_in.shape, F32),
            pltpu.VMEM((3,) + w_gate.shape, BF16),
            dma((5,)),
            pltpu.VMEM((pieces, 2 * units, width), BF16),
            pltpu.VMEM((n_mp * units - 2 * units, width), BF16),
            pltpu.VMEM((n_mp * units - 2 * units, width), BF16),
            pltpu.VMEM((n_mp, 2 * rank, units), F32),
            pltpu.VMEM((n_mp, lat, units), F32),
            pltpu.VMEM((n_mp, 2 * units, 6 * rank), BF16),
            pltpu.VMEM((4 * lat, n_mp * units), BF16),
            pltpu.VMEM((prompts, 6 * rank, share), BF16),
            pltpu.VMEM((pieces, n_z, lat, width), F32),
            pltpu.VMEM((pieces, lat, width), F32),
            pltpu.VMEM((pieces, 2, n_mp, lat, width), F32),
            pltpu.VMEM((prompts, 4, 128), F32),
            dma((2,)), dma((4,)),
            dma((1,)), dma((pieces,)),
            dma((3,)), dma((pieces + DIRECT,)),
            dma((1,)), dma((1,)),
            pltpu.SemaphoreType.REGULAR,
        ],
        compiler_params=pltpu.CompilerParams(collective_id=0, has_side_effects=True, vmem_limit_bytes=60000 * 1024),
    )(latents, noise, start_step, slide, table, w_in, w_gate, w_value, w_down, w_out.T)


def solution(mesh):
    in_specs = (
        P(None, "tm", None, None),
        P(None, "tm", None, None),
        P(),
        P(),
        P(),
        P(None, "mp"),
        P(None, "mp"),
        P("mp", None),
        P(),
    )
    out_specs = (P(None, "tm", None, None), P(None, "tm", None, "mp"))
    body = functools.partial(shards, mesh.shape["tm"], mesh.shape["mp"])
    return jax.shard_map(body, mesh=mesh, in_specs=in_specs, out_specs=out_specs, check_vma=False)
```

```python
import functools
import math

import jax
import jax.numpy as jnp
import numpy as np
from jax import lax
from jax.experimental import pallas as pl
from jax.experimental.pallas import tpu as pltpu
from jax.sharding import PartitionSpec as P

TSTEPS = 1000
DIRECT = 2
LAG = 3
F32, BF16 = jnp.float32, jnp.bfloat16
HIGH = lax.Precision.HIGHEST


def step_table(channels):
    beta = 1e-4 + (0.02 - 1e-4) * np.arange(TSTEPS, dtype=np.float64) / (TSTEPS - 1)
    abar = np.cumprod(1.0 - beta)
    root = np.sqrt(1.0 - beta)
    half = channels // 2
    freq = np.exp(-math.log(10000.0) * np.arange(half, dtype=np.float64) / half)
    table = np.zeros((4, max(TSTEPS, channels)), np.float32)
    table[:3, :TSTEPS] = [1.0 / root - 1.0, beta / np.sqrt(1.0 - abar) / root, np.sqrt(beta)]
    table[3, :channels] = np.concatenate([freq, freq])
    return table


def split3(v):
    a = v.astype(BF16).astype(F32)
    rest = v - a
    b = rest.astype(BF16).astype(F32)
    return a, b, rest - b


def six(parts, left):
    a, b, c = parts
    return jnp.concatenate([a, b, c, a, b, a] if left else [a, a, a, b, b, c], axis=0)


def contract(a, b, da, db, **kw):
    return lax.dot_general(a, b, (((da,), (db,)), ((), ())), preferred_element_type=F32, **kw)


def kernel(n_tm, n_mp, width, x_hbm, z_hbm, start_hbm, slide_hbm, table_hbm, win_hbm, wg_hbm, wv_hbm, wd_hbm, wo_hbm,
           out_ref, eps_ref, plan_ref, xz_ref, table_ref, io_ref, w_ref, load, hown, even, odd, wbuf, fbuf, a_scr, f_scr, y_scr, dbuf, obuf, pbuf,
           coef, wsend, wrecv, dsend, drecv, psend, precv, rsend, rrecv, zsem):
    prompts, _, lat, pos = x_hbm.shape
    units = w_ref.shape[2]
    rank = lat + prompts
    share = pos // n_mp
    cuts = share // width
    pieces = prompts * cuts
    n_z = n_tm // 2
    tm, mp = lax.axis_index("tm"), lax.axis_index("mp")
    zi, yi = lax.div(tm, 2), lax.rem(tm, 2)
    twin = tm + 1 - 2 * yi
    mesh_id = pl.DeviceIdType.MESH
    cols = pl.ds(pl.multiple_of(mp * share, 128), share)

    groups = [[(start_hbm, plan_ref.at[0]), (slide_hbm, plan_ref.at[1])],
              [(table_hbm, table_ref)],
              [(win_hbm, io_ref.at[0]), (wo_hbm, io_ref.at[1])],
              [(ref.at[pl.ds(r, units // 4)], w_ref.at[i, pl.ds(r, units // 4)]) for i, ref in enumerate((wg_hbm, wv_hbm, wd_hbm))
               for r in range(0, units, units // 4)],
              [(x_hbm.at[:, :, :, cols], xz_ref.at[0]), (z_hbm.at[:, :, :, cols], xz_ref.at[1])]]
    for i, group in enumerate(groups):
        for a, b in group:
            pltpu.make_async_copy(a, b, load.at[i]).start()
    whole = [pltpu.make_async_copy(a, a, load.at[i]) for i, a in enumerate((plan_ref, table_ref, io_ref, w_ref, xz_ref))]
    barrier = pltpu.get_barrier_semaphore()

    def peer(k):
        at = mp
        for b in range(k.bit_length()):
            if k >> b & 1:
                at = at + (1 << b) * (1 - 2 * lax.rem(lax.div(mp, 1 << b), 2))
        return at

    def greet(device):
        pl.semaphore_signal(barrier, inc=1, device_id=device, device_id_type=mesh_id)

    lax.fori_loop(zi + 1, n_z, lambda z, c: (greet({"tm": 2 * z + yi}), c)[1], 0)
    for k in range(1, n_mp):
        greet({"mp": peer(k)})
    for k in range(n_mp):
        greet({"tm": twin, "mp": peer(k)})

    for one in whole[:3]:
        one.wait()
    channels = io_ref.shape[2]
    order = lax.broadcasted_iota(jnp.int32, (prompts, channels), 0)
    times = jnp.zeros((prompts, channels), F32)
    for p in range(prompts):
        times = jnp.where(order == p, (plan_ref[0, p] - tm).astype(F32), times)
    angle = times * table_ref[3:4, :channels]
    lane = lax.broadcasted_iota(jnp.int32, (prompts, channels), 1)
    emb = jnp.where(lane < channels // 2, jnp.cos(angle), jnp.sin(angle))
    raw = jnp.concatenate([io_ref[0], emb], axis=0)
    left = raw - jnp.mean(raw, axis=1, keepdims=True)
    l3 = jnp.concatenate(split3(left), axis=0).astype(BF16)

    def folded(weights, width, db):
        got = contract(l3 if db == 0 else o3, weights, 1, db)
        return got[:width] + got[width:2 * width] + got[2 * width:3 * width]

    wot = io_ref[1]
    o3 = jnp.concatenate(split3(wot) + (jnp.zeros_like(wot),), axis=0).astype(BF16)
    root = math.sqrt(0.5)
    whole[3].wait()
    wbuf[0, 0:rank] = folded(w_ref[0], rank, 0) * root
    wbuf[0, rank:2 * rank] = folded(w_ref[1], rank, 0) * root
    fbuf[0] = folded(w_ref[2], lat, 1)

    def build(k):
        for part in range(2):
            a, b, c = split3(wbuf[k, part * rank:(part + 1) * rank])
            a_scr[k, part * units:(part + 1) * units] = six((a, b, c), True).T.astype(BF16)

    def build_down(k):
        a, b, c = split3(fbuf[k])
        f_scr[:, k * units:(k + 1) * units] = jnp.concatenate([a, b, c, jnp.zeros_like(a)], axis=0).astype(BF16)

    grid = lax.broadcasted_iota(jnp.int32, table_ref.shape, 1)
    for p in range(prompts):
        picked = jnp.where(grid == plan_ref[0, p] - tm, table_ref[...], 0.0)
        coef[p] = jnp.broadcast_to(jnp.sum(picked, axis=1, keepdims=True), coef.shape[1:])

    base = contract(raw, wot, 1, 1, precision=HIGH)
    base6 = six(split3(base), True).T.astype(BF16)
    gram = contract(left, left, 1, 1, precision=HIGH) * (1.0 / channels)
    gram6 = six(split3(gram), True).T.astype(BF16)
    rows = lax.broadcasted_iota(jnp.int32, (prompts, share), 0)
    whole[4].wait()
    for p in range(prompts):
        u = jnp.concatenate([xz_ref[0, p, 0], (rows == p).astype(F32)], axis=0)
        u6 = six(split3(u), False).astype(BF16)
        gu = jnp.dot(gram6, u6, preferred_element_type=F32)
        eps_ref[p, 0] = jnp.dot(base6, u6, preferred_element_type=F32)
        var = jnp.maximum(jnp.sum(gu * u, axis=0, keepdims=True), 0.0)
        y_scr[p] = six(split3(u * lax.rsqrt(var + 1e-5)), False).astype(BF16)

    def split(q):
        return lax.div(q, cuts), pl.ds(pl.multiple_of(lax.rem(q, cuts) * width, 128), width)

    def gated(k, yt, beside=iter(())):
        next(beside, None)
        gate = jnp.dot(a_scr[k, :units], yt, preferred_element_type=F32)
        next(beside, None)
        value = jnp.dot(a_scr[k, units:], yt, preferred_element_type=F32)
        return ((gate * (1.0 + lax.erf(gate))) * value).astype(BF16)

    def early(q, k):
        p, at = split(q)
        hown[q, k * units:(k + 1) * units] = gated(k, y_scr[p, :, at])

    def sweep(q, hid, beside=iter(())):
        p, at = split(q)
        yt = y_scr[p, :, at]
        for k in range(2, n_mp):
            hid[(k - 2) * units:(k - 1) * units] = gated(k, yt, beside)

    def remote(src, dst, send, recv, device):
        return pltpu.make_async_remote_copy(src, dst, send, recv, device_id=device, device_id_type=mesh_id)

    def bulk(ref, sem):
        return remote(ref, ref, sem, sem, {"mp": peer(1)})

    def drift_copy(q, z):
        return remote(dbuf.at[q, zi], dbuf.at[q, zi], dsend.at[0], drecv.at[q], {"tm": 2 * z + yi})

    def tiles(q, hid, got, begin=0):
        early_rows = 2 * units
        for low in range(begin, n_mp * units, 256):
            high = min(low + 256, n_mp * units)
            parts = []
            if low < early_rows:
                parts.append(hown[q, low:min(high, early_rows)])
            if high > early_rows:
                parts.append(hid[max(low - early_rows, 0):high - early_rows])
            block = parts[0] if len(parts) == 1 else jnp.concatenate(parts, axis=0)
            got.append(jnp.dot(f_scr[:, low:high], block, preferred_element_type=F32))
            yield

    def send(q, low, high):
        lax.fori_loop(low, high, lambda k, c: (drift_copy(q, k + jnp.where(k >= zi, 1, 0)).start(), c)[1], 0)

    def step(q, got):
        p, at = split(q)
        got = sum(got[1:], got[0])
        eps = eps_ref[p, 0, :, at] + got[:lat] + got[lat:2 * lat] + got[2 * lat:3 * lat]
        eps_ref[p, 0, :, at] = eps
        x = xz_ref[0, p, 0, :, at]
        c = coef[p]
        term = c[0:1, :1] * x - c[1:2, :1] * eps + c[2:3, :1] * xz_ref[1, p, 0, :, at]
        dbuf[q, zi] = term + jnp.where(tm == 0, 1.0, 0.0) * x
        if q == 0:
            @pl.when(zi < n_z - 1)
            def _():
                pl.semaphore_wait(zsem, n_z - 1 - zi)

        some = jnp.where(tm == n_tm - 1, 0, 1)
        send(q, 0, some)
        send(q, jnp.maximum(zi, 1), n_z - 1)
        for r in range(max(q - LAG, 0), q - LAG + 1 if q < pieces - 1 else pieces):
            send(r, 1, 1 + some * (jnp.maximum(zi, 1) - 1))

    def place(q, owner):
        return pl.ds(pl.multiple_of(owner * share + lax.rem(q, cuts) * width, 128), width)

    def own_copy(q, k, sem=0):
        spot = pbuf.at[q, yi, mp]
        return remote(spot, spot, psend.at[sem], precv.at[q], {"mp": peer(k)})

    def twin_copy(q, k, sem=0, arrive=None):
        return remote(obuf.at[q], pbuf.at[q, yi, mp], psend.at[sem], precv.at[q if arrive is None else arrive], {"tm": twin, "mp": peer(k)})

    def merge(q):
        short = (yi == 1) & (zi < n_z - 1)

        @pl.when(short)
        def _():
            bulk(dbuf.at[q, pl.ds(0, n_z - 2)], drecv.at[q]).wait_recv()

        @pl.when(jnp.logical_not(short))
        def _():
            bulk(dbuf.at[q, pl.ds(0, n_z - 1)], drecv.at[q]).wait_recv()

        p = lax.div(q, cuts)
        mine = jnp.minimum(tm + plan_ref[1, p], n_tm - 1)
        theirs = jnp.minimum(twin + plan_ref[1, p], n_tm - 1)

        def add(z, totals):
            part = dbuf[q, z]
            slot = 2 * z + yi
            return (totals[0] + jnp.where(slot < mine, 1.0, 0.0) * part,
                    totals[1] + jnp.where(slot < theirs, 1.0, 0.0) * part)

        zero = jnp.zeros((lat, width), F32)
        sums = lax.fori_loop(0, n_z - 1, add, (zero, zero), unroll=n_z <= 8)
        keep, give = lax.fori_loop(n_z - 1, n_z - yi, add, sums)
        pbuf[q, yi, mp] = keep
        obuf[q] = give

    def by_side(first, second):
        @pl.when(yi == 0)
        def _():
            first()
            second()

        @pl.when(yi == 1)
        def _():
            second()
            first()

    def finish(q):
        merge(q)

        def own():
            for k in range(2, n_mp, 2):
                own_copy(q, k).start()

        def other():
            for k in range(0, n_mp, 2):
                twin_copy(q, k).start()

        by_side(own, other)

    def finish_direct(q):
        merge(q)

        def own():
            for k in range(n_mp - 1, 0, -1):
                own_copy(q, k, 1).start()

        def other():
            for k in range(n_mp - 1, -1, -1):
                twin_copy(q, k, 2, q + DIRECT).start()

        by_side(own, other)

    def gather_direct(q):
        p = lax.div(q, cuts)
        bulk(pbuf.at[q, 0, pl.ds(0, n_mp - 1)], precv.at[q]).wait_recv()
        bulk(pbuf.at[q, 1], precv.at[q + DIRECT]).wait_recv()
        for owner in range(n_mp):
            out_ref[p, 0, :, place(q, owner)] = pbuf[q, 0, owner] + pbuf[q, 1, owner]

    def relay(q):
        p = lax.div(q, cuts)
        bulk(pbuf.at[q, 0, pl.ds(0, n_mp - 1)], precv.at[q]).wait_recv()
        for k in range(0, n_mp, 2):
            owner = peer(k)
            at = place(q, owner)
            out_ref[p, 0, :, at] = pbuf[q, 0, owner] + pbuf[q, 1, owner]
            spot = out_ref.at[p, 0, :, at]
            remote(spot, spot, rsend.at[0], rrecv.at[0], {"mp": peer(1)}).start()

    def loop(count, op, start=0):
        lax.fori_loop(start, count, lambda q, c: (op(q), c)[1], 0)

    def table_copy(k, ref, at):
        return remote(ref.at[0], ref.at[k], wsend.at[at], wrecv.at[2 * at + min(k, 2) - 1], {"mp": peer(k)})

    build(0)
    build_down(0)
    pl.semaphore_wait(barrier, zi + n_mp - 1 + n_mp)

    def reply(z, c):
        pl.semaphore_signal(zsem, inc=1, device_id={"tm": 2 * z + yi}, device_id_type=mesh_id)
        return c

    lax.fori_loop(0, zi, reply, 0)
    order_k = list(range(1, n_mp))
    for k in order_k:
        table_copy(k, wbuf, 0).start()
    for k in order_k:
        table_copy(k, fbuf, 1).start()

    for q in range(pieces):
        early(q, 0)

    bulk(wbuf.at[1], wrecv.at[0]).wait_recv()
    bulk(fbuf.at[1], wrecv.at[2]).wait_recv()
    build(1)
    build_down(1)
    for q in range(pieces):
        early(q, 1)
    bulk(wbuf.at[pl.ds(2, n_mp - 2)], wrecv.at[1]).wait_recv()
    for k in range(2, n_mp):
        build(k)
    bulk(fbuf.at[pl.ds(2, n_mp - 2)], wrecv.at[3]).wait_recv()
    for k in range(2, n_mp):
        build_down(k)

    bufs = (even, odd)
    sweep(0, even)
    ripe = 2 * units // 256 * 256

    def ripened(q, got):
        for low in range(0, ripe, 256):
            got.append(jnp.dot(f_scr[:, low:low + 256], hown[q, low:low + 256], preferred_element_type=F32))

    for q in range(1, pieces):
        got, ahead = [], []
        beside = tiles(q - 1, bufs[(q - 1) % 2], got)
        if q == pieces - 1:
            ripened(q, ahead)
        sweep(q, bufs[q % 2], beside)
        for _ in beside:
            pass
        step(q - 1, got)
    for _ in tiles(pieces - 1, bufs[(pieces - 1) % 2], ahead, ripe):
        pass
    step(pieces - 1, ahead)

    loop(pieces - DIRECT, finish)
    loop(pieces, finish_direct, pieces - DIRECT)
    loop(pieces - DIRECT, relay)
    loop(pieces, gather_direct, pieces - DIRECT)

    half = pbuf.at[pl.ds(0, pieces - DIRECT), 0, pl.ds(0, n_mp // 2)]
    bulk(half, rrecv.at[0]).wait_recv()
    bulk(half, rsend.at[0]).wait_send()
    bulk(wbuf.at[pl.ds(1, n_mp - 1)], wsend.at[0]).wait_send()
    bulk(fbuf.at[pl.ds(1, n_mp - 1)], wsend.at[1]).wait_send()

    @pl.when(tm != n_tm - 1)
    def _():
        bulk(dbuf.at[:, pl.ds(0, n_z - 1)], dsend.at[0]).wait_send()

    bulk(pbuf.at[pl.ds(0, pieces - DIRECT), 0, pl.ds(0, n_mp - 1)], psend.at[0]).wait_send()
    bulk(pbuf.at[pl.ds(0, DIRECT), 0, pl.ds(0, n_mp - 1)], psend.at[1]).wait_send()
    bulk(pbuf.at[pl.ds(0, DIRECT), 0], psend.at[2]).wait_send()


def shards(n_tm, n_mp, latents, noise, start_step, slide, w_in, w_gate, w_value, w_down, w_out):
    prompts, t_dev, lat, pos = latents.shape
    channels, units = w_gate.shape
    share = pos // n_mp
    rank = lat + prompts
    width = 512
    pieces = prompts * share // width
    n_z = n_tm // 2
    assert w_gate.shape == w_down.shape and t_dev == 1 and n_tm % 2 == 0 and pieces % 2 == 0 and n_mp > 2 and n_mp & (n_mp - 1) == 0
    vmem = pl.BlockSpec(memory_space=pltpu.VMEM)
    dma = pltpu.SemaphoreType.DMA
    hbm = pl.BlockSpec(memory_space=pltpu.HBM)
    table = step_table(channels)
    return pl.pallas_call(
        functools.partial(kernel, n_tm, n_mp, width),
        out_shape=(pltpu.VMEM(latents.shape, F32), pltpu.VMEM((prompts, 1, lat, share), F32)),
        in_specs=[hbm] * 10,
        out_specs=(vmem, vmem),
        scratch_shapes=[
            pltpu.SMEM((2, prompts), jnp.int32),
            pltpu.VMEM((2, prompts, 1, lat, share), F32),
            pltpu.VMEM(table.shape, F32),
            pltpu.VMEM((2,) + w_in.shape, F32),
            pltpu.VMEM((3,) + w_gate.shape, BF16),
            dma((5,)),
            pltpu.VMEM((pieces, 2 * units, width), BF16),
            pltpu.VMEM((n_mp * units - 2 * units, width), BF16),
            pltpu.VMEM((n_mp * units - 2 * units, width), BF16),
            pltpu.VMEM((n_mp, 2 * rank, units), F32),
            pltpu.VMEM((n_mp, lat, units), F32),
            pltpu.VMEM((n_mp, 2 * units, 6 * rank), BF16),
            pltpu.VMEM((4 * lat, n_mp * units), BF16),
            pltpu.VMEM((prompts, 6 * rank, share), BF16),
            pltpu.VMEM((pieces, n_z, lat, width), F32),
            pltpu.VMEM((pieces, lat, width), F32),
            pltpu.VMEM((pieces, 2, n_mp, lat, width), F32),
            pltpu.VMEM((prompts, 4, 128), F32),
            dma((2,)), dma((4,)),
            dma((1,)), dma((pieces,)),
            dma((3,)), dma((pieces + DIRECT,)),
            dma((1,)), dma((1,)),
            pltpu.SemaphoreType.REGULAR,
        ],
        compiler_params=pltpu.CompilerParams(collective_id=0, has_side_effects=True, vmem_limit_bytes=60000 * 1024),
    )(latents, noise, start_step, slide, table, w_in, w_gate, w_value, w_down, w_out.T)


def solution(mesh):
    in_specs = (
        P(None, "tm", None, None),
        P(None, "tm", None, None),
        P(),
        P(),
        P(),
        P(None, "mp"),
        P(None, "mp"),
        P("mp", None),
        P(),
    )
    out_specs = (P(None, "tm", None, None), P(None, "tm", None, "mp"))
    body = functools.partial(shards, mesh.shape["tm"], mesh.shape["mp"])
    return jax.shard_map(body, mesh=mesh, in_specs=in_specs, out_specs=out_specs, check_vma=False)
```

```python
import functools
import math

import jax
import jax.numpy as jnp
import numpy as np
from jax import lax
from jax.experimental import pallas as pl
from jax.experimental.pallas import tpu as pltpu
from jax.sharding import PartitionSpec as P

TSTEPS = 1000
DIRECT = 3
LAG = 4
F32, BF16 = jnp.float32, jnp.bfloat16
HIGH = lax.Precision.HIGHEST


def step_table(channels):
    beta = 1e-4 + (0.02 - 1e-4) * np.arange(TSTEPS, dtype=np.float64) / (TSTEPS - 1)
    abar = np.cumprod(1.0 - beta)
    root = np.sqrt(1.0 - beta)
    half = channels // 2
    freq = np.exp(-math.log(10000.0) * np.arange(half, dtype=np.float64) / half)
    table = np.zeros((4, max(TSTEPS, channels)), np.float32)
    table[:3, :TSTEPS] = [1.0 / root - 1.0, beta / np.sqrt(1.0 - abar) / root, np.sqrt(beta)]
    table[3, :channels] = np.concatenate([freq, freq])
    return table


def split3(v):
    a = v.astype(BF16).astype(F32)
    rest = v - a
    b = rest.astype(BF16).astype(F32)
    return a, b, rest - b


def six(parts, left):
    a, b, c = parts
    return jnp.concatenate([a, b, c, a, b, a] if left else [a, a, a, b, b, c], axis=0)


def contract(a, b, da, db, **kw):
    return lax.dot_general(a, b, (((da,), (db,)), ((), ())), preferred_element_type=F32, **kw)


def kernel(n_tm, n_mp, width, x_hbm, z_hbm, start_hbm, slide_hbm, table_hbm, win_hbm, wg_hbm, wv_hbm, wd_hbm, wo_hbm,
           out_ref, eps_ref, plan_ref, xz_ref, table_ref, io_ref, w_ref, load, hown, even, odd, wbuf, fbuf, a_scr, f_scr, y_scr, dbuf, obuf, pbuf,
           coef, wsend, wrecv, dsend, drecv, psend, precv, rsend, rrecv, zsem):
    prompts, _, lat, pos = x_hbm.shape
    units = w_ref.shape[2]
    rank = lat + prompts
    share = pos // n_mp
    cuts = share // width
    pieces = prompts * cuts
    n_z = n_tm // 2
    tm, mp = lax.axis_index("tm"), lax.axis_index("mp")
    zi, yi = lax.div(tm, 2), lax.rem(tm, 2)
    twin = tm + 1 - 2 * yi
    mesh_id = pl.DeviceIdType.MESH
    cols = pl.ds(pl.multiple_of(mp * share, 128), share)

    groups = [[(start_hbm, plan_ref.at[0]), (slide_hbm, plan_ref.at[1])],
              [(table_hbm, table_ref)],
              [(win_hbm, io_ref.at[0]), (wo_hbm, io_ref.at[1])],
              [(ref.at[pl.ds(r, units // 4)], w_ref.at[i, pl.ds(r, units // 4)]) for i, ref in enumerate((wg_hbm, wv_hbm, wd_hbm))
               for r in range(0, units, units // 4)],
              [(x_hbm.at[:, :, :, cols], xz_ref.at[0]), (z_hbm.at[:, :, :, cols], xz_ref.at[1])]]
    for i, group in enumerate(groups):
        for a, b in group:
            pltpu.make_async_copy(a, b, load.at[i]).start()
    whole = [pltpu.make_async_copy(a, a, load.at[i]) for i, a in enumerate((plan_ref, table_ref, io_ref, w_ref, xz_ref))]
    barrier = pltpu.get_barrier_semaphore()

    def peer(k):
        at = mp
        for b in range(k.bit_length()):
            if k >> b & 1:
                at = at + (1 << b) * (1 - 2 * lax.rem(lax.div(mp, 1 << b), 2))
        return at

    def greet(device):
        pl.semaphore_signal(barrier, inc=1, device_id=device, device_id_type=mesh_id)

    lax.fori_loop(zi + 1, n_z, lambda z, c: (greet({"tm": 2 * z + yi}), c)[1], 0)
    for k in range(1, n_mp):
        greet({"mp": peer(k)})
    for k in range(n_mp):
        greet({"tm": twin, "mp": peer(k)})

    for one in whole[:3]:
        one.wait()
    channels = io_ref.shape[2]
    order = lax.broadcasted_iota(jnp.int32, (prompts, channels), 0)
    times = jnp.zeros((prompts, channels), F32)
    for p in range(prompts):
        times = jnp.where(order == p, (plan_ref[0, p] - tm).astype(F32), times)
    angle = times * table_ref[3:4, :channels]
    lane = lax.broadcasted_iota(jnp.int32, (prompts, channels), 1)
    emb = jnp.where(lane < channels // 2, jnp.cos(angle), jnp.sin(angle))
    raw = jnp.concatenate([io_ref[0], emb], axis=0)
    left = raw - jnp.mean(raw, axis=1, keepdims=True)
    l3 = jnp.concatenate(split3(left), axis=0).astype(BF16)

    def folded(weights, width, db):
        got = contract(l3 if db == 0 else o3, weights, 1, db)
        return got[:width] + got[width:2 * width] + got[2 * width:3 * width]

    wot = io_ref[1]
    o3 = jnp.concatenate(split3(wot) + (jnp.zeros_like(wot),), axis=0).astype(BF16)
    root = math.sqrt(0.5)
    whole[3].wait()
    wbuf[0, 0:rank] = folded(w_ref[0], rank, 0) * root
    wbuf[0, rank:2 * rank] = folded(w_ref[1], rank, 0) * root
    fbuf[0] = folded(w_ref[2], lat, 1)

    def build(k):
        for part in range(2):
            a, b, c = split3(wbuf[k, part * rank:(part + 1) * rank])
            a_scr[k, part * units:(part + 1) * units] = six((a, b, c), True).T.astype(BF16)

    def build_down(k):
        a, b, c = split3(fbuf[k])
        f_scr[:, k * units:(k + 1) * units] = jnp.concatenate([a, b, c, jnp.zeros_like(a)], axis=0).astype(BF16)

    grid = lax.broadcasted_iota(jnp.int32, table_ref.shape, 1)
    for p in range(prompts):
        picked = jnp.where(grid == plan_ref[0, p] - tm, table_ref[...], 0.0)
        coef[p] = jnp.broadcast_to(jnp.sum(picked, axis=1, keepdims=True), coef.shape[1:])

    base = contract(raw, wot, 1, 1, precision=HIGH)
    base6 = six(split3(base), True).T.astype(BF16)
    gram = contract(left, left, 1, 1, precision=HIGH) * (1.0 / channels)
    gram6 = six(split3(gram), True).T.astype(BF16)
    rows = lax.broadcasted_iota(jnp.int32, (prompts, share), 0)
    whole[4].wait()
    for p in range(prompts):
        u = jnp.concatenate([xz_ref[0, p, 0], (rows == p).astype(F32)], axis=0)
        u6 = six(split3(u), False).astype(BF16)
        gu = jnp.dot(gram6, u6, preferred_element_type=F32)
        eps_ref[p, 0] = jnp.dot(base6, u6, preferred_element_type=F32)
        var = jnp.maximum(jnp.sum(gu * u, axis=0, keepdims=True), 0.0)
        y_scr[p] = six(split3(u * lax.rsqrt(var + 1e-5)), False).astype(BF16)

    def split(q):
        return lax.div(q, cuts), pl.ds(pl.multiple_of(lax.rem(q, cuts) * width, 128), width)

    def gated(k, yt, beside=iter(())):
        next(beside, None)
        gate = jnp.dot(a_scr[k, :units], yt, preferred_element_type=F32)
        next(beside, None)
        value = jnp.dot(a_scr[k, units:], yt, preferred_element_type=F32)
        return ((gate * (1.0 + lax.erf(gate))) * value).astype(BF16)

    def early(q, k):
        p, at = split(q)
        hown[q, k * units:(k + 1) * units] = gated(k, y_scr[p, :, at])

    def sweep(q, hid, beside=iter(())):
        p, at = split(q)
        yt = y_scr[p, :, at]
        for k in range(2, n_mp):
            hid[(k - 2) * units:(k - 1) * units] = gated(k, yt, beside)

    def remote(src, dst, send, recv, device):
        return pltpu.make_async_remote_copy(src, dst, send, recv, device_id=device, device_id_type=mesh_id)

    def bulk(ref, sem):
        return remote(ref, ref, sem, sem, {"mp": peer(1)})

    def drift_copy(q, z):
        return remote(dbuf.at[q, zi], dbuf.at[q, zi], dsend.at[0], drecv.at[q], {"tm": 2 * z + yi})

    def tiles(q, hid, got, begin=0):
        early_rows = 2 * units
        for low in range(begin, n_mp * units, 256):
            high = min(low + 256, n_mp * units)
            parts = []
            if low < early_rows:
                parts.append(hown[q, low:min(high, early_rows)])
            if high > early_rows:
                parts.append(hid[max(low - early_rows, 0):high - early_rows])
            block = parts[0] if len(parts) == 1 else jnp.concatenate(parts, axis=0)
            got.append(jnp.dot(f_scr[:, low:high], block, preferred_element_type=F32))
            yield

    def send(q, low, high):
        lax.fori_loop(low, high, lambda k, c: (drift_copy(q, k + jnp.where(k >= zi, 1, 0)).start(), c)[1], 0)

    def step(q, got):
        p, at = split(q)
        got = sum(got[1:], got[0])
        eps = eps_ref[p, 0, :, at] + got[:lat] + got[lat:2 * lat] + got[2 * lat:3 * lat]
        eps_ref[p, 0, :, at] = eps
        x = xz_ref[0, p, 0, :, at]
        c = coef[p]
        term = c[0:1, :1] * x - c[1:2, :1] * eps + c[2:3, :1] * xz_ref[1, p, 0, :, at]
        dbuf[q, zi] = term + jnp.where(tm == 0, 1.0, 0.0) * x
        if q == 0:
            @pl.when(zi < n_z - 1)
            def _():
                pl.semaphore_wait(zsem, n_z - 1 - zi)

        some = jnp.where(tm == n_tm - 1, 0, 1)
        send(q, 0, some)
        send(q, jnp.maximum(zi, 1), n_z - 1)
        for r in range(max(q - LAG, 0), q - LAG + 1 if q < pieces - 1 else pieces):
            send(r, 1, 1 + some * (jnp.maximum(zi, 1) - 1))

    def place(q, owner):
        return pl.ds(pl.multiple_of(owner * share + lax.rem(q, cuts) * width, 128), width)

    def own_copy(q, k, sem=0):
        spot = pbuf.at[q, yi, mp]
        return remote(spot, spot, psend.at[sem], precv.at[q], {"mp": peer(k)})

    def twin_copy(q, k, sem=0, arrive=None):
        return remote(obuf.at[q], pbuf.at[q, yi, mp], psend.at[sem], precv.at[q if arrive is None else arrive], {"tm": twin, "mp": peer(k)})

    def merge(q):
        short = (yi == 1) & (zi < n_z - 1)

        @pl.when(short)
        def _():
            bulk(dbuf.at[q, pl.ds(0, n_z - 2)], drecv.at[q]).wait_recv()

        @pl.when(jnp.logical_not(short))
        def _():
            bulk(dbuf.at[q, pl.ds(0, n_z - 1)], drecv.at[q]).wait_recv()

        p = lax.div(q, cuts)
        mine = jnp.minimum(tm + plan_ref[1, p], n_tm - 1)
        theirs = jnp.minimum(twin + plan_ref[1, p], n_tm - 1)

        def add(z, totals):
            part = dbuf[q, z]
            slot = 2 * z + yi
            return (totals[0] + jnp.where(slot < mine, 1.0, 0.0) * part,
                    totals[1] + jnp.where(slot < theirs, 1.0, 0.0) * part)

        zero = jnp.zeros((lat, width), F32)
        sums = lax.fori_loop(0, n_z - 1, add, (zero, zero), unroll=n_z <= 8)
        keep, give = lax.fori_loop(n_z - 1, n_z - yi, add, sums)
        pbuf[q, yi, mp] = keep
        obuf[q] = give

    def by_side(first, second):
        @pl.when(yi == 0)
        def _():
            first()
            second()

        @pl.when(yi == 1)
        def _():
            second()
            first()

    def finish(q):
        merge(q)

        def own():
            for k in range(2, n_mp, 2):
                own_copy(q, k).start()

        def other():
            for k in range(0, n_mp, 2):
                twin_copy(q, k).start()

        by_side(own, other)

    def finish_direct(q):
        merge(q)

        def own():
            for k in range(n_mp - 1, 0, -1):
                own_copy(q, k, 1).start()

        def other():
            for k in range(n_mp - 1, -1, -1):
                twin_copy(q, k, 2, q + DIRECT).start()

        by_side(own, other)

    def gather_direct(q):
        p = lax.div(q, cuts)
        bulk(pbuf.at[q, 0, pl.ds(0, n_mp - 1)], precv.at[q]).wait_recv()
        bulk(pbuf.at[q, 1], precv.at[q + DIRECT]).wait_recv()
        for owner in range(n_mp):
            out_ref[p, 0, :, place(q, owner)] = pbuf[q, 0, owner] + pbuf[q, 1, owner]

    def relay(q):
        p = lax.div(q, cuts)
        bulk(pbuf.at[q, 0, pl.ds(0, n_mp - 1)], precv.at[q]).wait_recv()
        for k in range(0, n_mp, 2):
            owner = peer(k)
            at = place(q, owner)
            out_ref[p, 0, :, at] = pbuf[q, 0, owner] + pbuf[q, 1, owner]
            spot = out_ref.at[p, 0, :, at]
            remote(spot, spot, rsend.at[0], rrecv.at[0], {"mp": peer(1)}).start()

    def loop(count, op, start=0):
        lax.fori_loop(start, count, lambda q, c: (op(q), c)[1], 0)

    def table_copy(k, ref, at):
        return remote(ref.at[0], ref.at[k], wsend.at[at], wrecv.at[2 * at + min(k, 2) - 1], {"mp": peer(k)})

    build(0)
    build_down(0)
    pl.semaphore_wait(barrier, zi + n_mp - 1 + n_mp)

    def reply(z, c):
        pl.semaphore_signal(zsem, inc=1, device_id={"tm": 2 * z + yi}, device_id_type=mesh_id)
        return c

    lax.fori_loop(0, zi, reply, 0)
    order_k = list(range(1, n_mp))
    for k in order_k:
        table_copy(k, wbuf, 0).start()
    for k in order_k:
        table_copy(k, fbuf, 1).start()

    for q in range(pieces):
        early(q, 0)

    bulk(wbuf.at[1], wrecv.at[0]).wait_recv()
    bulk(fbuf.at[1], wrecv.at[2]).wait_recv()
    build(1)
    build_down(1)
    for q in range(pieces):
        early(q, 1)
    bulk(wbuf.at[pl.ds(2, n_mp - 2)], wrecv.at[1]).wait_recv()
    for k in range(2, n_mp):
        build(k)
    bulk(fbuf.at[pl.ds(2, n_mp - 2)], wrecv.at[3]).wait_recv()
    for k in range(2, n_mp):
        build_down(k)

    bufs = (even, odd)
    sweep(0, even)
    ripe = 2 * units // 256 * 256

    def ripened(q, got):
        for low in range(0, ripe, 256):
            got.append(jnp.dot(f_scr[:, low:low + 256], hown[q, low:low + 256], preferred_element_type=F32))

    for q in range(1, pieces):
        got, ahead = [], []
        beside = tiles(q - 1, bufs[(q - 1) % 2], got)
        if q == pieces - 1:
            ripened(q, ahead)
        sweep(q, bufs[q % 2], beside)
        for _ in beside:
            pass
        step(q - 1, got)
    for _ in tiles(pieces - 1, bufs[(pieces - 1) % 2], ahead, ripe):
        pass
    step(pieces - 1, ahead)

    loop(pieces - DIRECT, finish)
    loop(pieces, finish_direct, pieces - DIRECT)
    loop(pieces - DIRECT, relay)
    loop(pieces, gather_direct, pieces - DIRECT)

    half = pbuf.at[pl.ds(0, pieces - DIRECT), 0, pl.ds(0, n_mp // 2)]
    bulk(half, rrecv.at[0]).wait_recv()
    bulk(half, rsend.at[0]).wait_send()
    bulk(wbuf.at[pl.ds(1, n_mp - 1)], wsend.at[0]).wait_send()
    bulk(fbuf.at[pl.ds(1, n_mp - 1)], wsend.at[1]).wait_send()

    @pl.when(tm != n_tm - 1)
    def _():
        bulk(dbuf.at[:, pl.ds(0, n_z - 1)], dsend.at[0]).wait_send()

    bulk(pbuf.at[pl.ds(0, pieces - DIRECT), 0, pl.ds(0, n_mp - 1)], psend.at[0]).wait_send()
    bulk(pbuf.at[pl.ds(0, DIRECT), 0, pl.ds(0, n_mp - 1)], psend.at[1]).wait_send()
    bulk(pbuf.at[pl.ds(0, DIRECT), 0], psend.at[2]).wait_send()


def shards(n_tm, n_mp, latents, noise, start_step, slide, w_in, w_gate, w_value, w_down, w_out):
    prompts, t_dev, lat, pos = latents.shape
    channels, units = w_gate.shape
    share = pos // n_mp
    rank = lat + prompts
    width = 512
    pieces = prompts * share // width
    n_z = n_tm // 2
    assert w_gate.shape == w_down.shape and t_dev == 1 and n_tm % 2 == 0 and pieces % 2 == 0 and n_mp > 2 and n_mp & (n_mp - 1) == 0
    vmem = pl.BlockSpec(memory_space=pltpu.VMEM)
    dma = pltpu.SemaphoreType.DMA
    hbm = pl.BlockSpec(memory_space=pltpu.HBM)
    table = step_table(channels)
    return pl.pallas_call(
        functools.partial(kernel, n_tm, n_mp, width),
        out_shape=(pltpu.VMEM(latents.shape, F32), pltpu.VMEM((prompts, 1, lat, share), F32)),
        in_specs=[hbm] * 10,
        out_specs=(vmem, vmem),
        scratch_shapes=[
            pltpu.SMEM((2, prompts), jnp.int32),
            pltpu.VMEM((2, prompts, 1, lat, share), F32),
            pltpu.VMEM(table.shape, F32),
            pltpu.VMEM((2,) + w_in.shape, F32),
            pltpu.VMEM((3,) + w_gate.shape, BF16),
            dma((5,)),
            pltpu.VMEM((pieces, 2 * units, width), BF16),
            pltpu.VMEM((n_mp * units - 2 * units, width), BF16),
            pltpu.VMEM((n_mp * units - 2 * units, width), BF16),
            pltpu.VMEM((n_mp, 2 * rank, units), F32),
            pltpu.VMEM((n_mp, lat, units), F32),
            pltpu.VMEM((n_mp, 2 * units, 6 * rank), BF16),
            pltpu.VMEM((4 * lat, n_mp * units), BF16),
            pltpu.VMEM((prompts, 6 * rank, share), BF16),
            pltpu.VMEM((pieces, n_z, lat, width), F32),
            pltpu.VMEM((pieces, lat, width), F32),
            pltpu.VMEM((pieces, 2, n_mp, lat, width), F32),
            pltpu.VMEM((prompts, 4, 128), F32),
            dma((2,)), dma((4,)),
            dma((1,)), dma((pieces,)),
            dma((3,)), dma((pieces + DIRECT,)),
            dma((1,)), dma((1,)),
            pltpu.SemaphoreType.REGULAR,
        ],
        compiler_params=pltpu.CompilerParams(collective_id=0, has_side_effects=True, vmem_limit_bytes=60000 * 1024),
    )(latents, noise, start_step, slide, table, w_in, w_gate, w_value, w_down, w_out.T)


def solution(mesh):
    in_specs = (
        P(None, "tm", None, None),
        P(None, "tm", None, None),
        P(),
        P(),
        P(),
        P(None, "mp"),
        P(None, "mp"),
        P("mp", None),
        P(),
    )
    out_specs = (P(None, "tm", None, None), P(None, "tm", None, "mp"))
    body = functools.partial(shards, mesh.shape["tm"], mesh.shape["mp"])
    return jax.shard_map(body, mesh=mesh, in_specs=in_specs, out_specs=out_specs, check_vma=False)
```
